32 devices in a mesh: dp: 4 (over x, y), sp: 8 (over z, core).
Axes of the slice: x: 2, y: 2, z: 4, core: 2. Of those that a mesh axis runs over, the one named last changes fastest.
Arguments:
- x: bfloat16 [16384, 4096], P(('dp', 'sp')), parts along dimension 0
- gain: bfloat16 [4096], replicated
- wq: bfloat16 [4096, 4096], P('sp')
- wk: bfloat16 [4096, 512], P('sp')
- wv: bfloat16 [4096, 512], P('sp')
- wo: bfloat16 [4096, 4096], P('sp')
Outputs:
- output: bfloat16 [16384, 4096], P(('dp', 'sp')), parts along dimension 0
There are 4 independent parts. The reference program is written for one: setup_inputs(seed, part) draws one part's arguments, and reference() takes and returns one part's arrays. A program takes and returns all parts, laid end to end along the dimension named above; an argument that names none is the same for every part.
All inputs are finite; a program needn't handle non-finite values.
Results may differ from the reference program's by a relative error of at most 0.012.
Values are sent between devices in bfloat16 or wider.
A program may use at most 2 GiB of HBM per device.

```python
import jax
import jax.numpy as jnp
from jax import lax

ROWS = 4096
D = 4096
HEADS = 32
KV_HEADS = 4
HEAD = 128
THETA = 10000


def setup_inputs(seed: int = 0, part: int = 0) -> dict:
    kx, kn, kq, kk, kv, ko = jax.random.split(jax.random.key(seed), 6)

    def weights(key, rows, columns):
        return jax.random.normal(key, (rows, columns), jnp.float32) * rows**-0.5

    drawn = {
        "x": jax.random.normal(jax.random.fold_in(kx, part), (ROWS, D), jnp.float32),
        "gain": 1 + 0.1 * jax.random.normal(kn, (D,), jnp.float32),
        "wq": 2 * weights(kq, D, HEADS * HEAD),
        "wk": 2 * weights(kk, D, KV_HEADS * HEAD),
        "wv": 4 * weights(kv, D, KV_HEADS * HEAD),
        "wo": weights(ko, HEADS * HEAD, D),
    }
    return {k: v.astype(jnp.bfloat16) for k, v in drawn.items()}


def normed(x, gain):
    wide = x.astype(jnp.float32)
    scale = lax.rsqrt(jnp.mean(wide * wide, -1, keepdims=True) + 1e-6)
    return (wide * scale * gain.astype(jnp.float32)).astype(jnp.bfloat16)


def turned(t, place, theta):
    half = t.shape[-1] // 2
    angle = place.astype(jnp.float32)[:, None] * theta ** (-jnp.arange(half, dtype=jnp.float32) / half)
    cos, sin = jnp.cos(angle)[:, None], jnp.sin(angle)[:, None]
    a, b = t[..., :half].astype(jnp.float32), t[..., half:].astype(jnp.float32)
    return jnp.concatenate([a * cos - b * sin, b * cos + a * sin], -1).astype(jnp.bfloat16)


def matmul(a, w):
    return jnp.dot(a, w, preferred_element_type=jnp.float32).astype(jnp.bfloat16)


def einsum(form, a, b):
    return jnp.einsum(form, a.astype(jnp.float32), b.astype(jnp.float32))


def attention(q, k, v):
    scores = einsum("tgsd,ugd->gstu", q, k) * q.shape[-1] ** -0.5
    token = jnp.arange(q.shape[0])
    scores = jnp.where(token[:, None] >= token, scores, -jnp.inf)
    weights = jax.nn.softmax(scores, -1).astype(jnp.bfloat16)
    return einsum("gstu,ugd->tgsd", weights, v).astype(jnp.bfloat16)


def reference(x, gain, wq, wk, wv, wo):
    a, place = normed(x, gain), jnp.arange(ROWS)
    q = turned(matmul(a, wq).reshape(ROWS, HEADS, HEAD), place, THETA).reshape(ROWS, KV_HEADS, -1, HEAD)
    k = turned(matmul(a, wk).reshape(ROWS, KV_HEADS, HEAD), place, THETA)
    v = matmul(a, wv).reshape(ROWS, KV_HEADS, HEAD)
    seen = attention(q, k, v).reshape(ROWS, HEADS * HEAD)
    return (x.astype(jnp.float32) + jnp.dot(seen, wo, preferred_element_type=jnp.float32)).astype(jnp.bfloat16)
```

```python
import functools

import jax
import jax.numpy as jnp
from jax import lax
from jax.experimental import pallas as pl
from jax.experimental.pallas import tpu as pltpu
from jax.sharding import PartitionSpec as P

MESH = pl.DeviceIdType.MESH
NEG = -1e30
HIDDEN = 2 * NEG
LOG2E = 1.4426950408889634
VMEM = 63 * 2**20
HEAD = 128
THETA = 10000
T = 512
D = 4096
HALF = 2048
QUARTER = T // 4
SLOTS = 12
F32 = jnp.float32
BF16 = jnp.bfloat16


def _dot(a, b, ca, cb):
    return lax.dot_general(a, b, (((ca,), (cb,)), ((), ())), preferred_element_type=F32)


def _kernel(x_ref, gain_ref, wkv_ref, wq_ref, wo_ref, cos_ref, sin_ref, y_ref, gkv_ref, g_ref,
            x_s, lhs_s, q_s, kv_s, acc_s, w_s, mix_s, top_s,
            rz, rx, ry, rdx, rdy, rs, sz, sx, sy, sdx, sdy, ss, sup, sdown, sown,
            rkv, rskv, skv_up, skv_sib, skv_own, load_sem, small_sem, y_sem):
    dp, sp = lax.axis_index("dp"), lax.axis_index("sp")
    xq, yq = dp // 2, dp % 2
    z, c = sp // 2, sp % 2
    dpx, dpy = (1 - xq) * 2 + yq, xq * 2 + (1 - yq)
    dpd = 3 - dp
    to_x, to_y, to_sib = (dpx, sp), (dpy, sp), (dp, z * 2 + (1 - c))
    to_up, to_down = (dp, sp + 2), (dp, sp - 2)

    barrier = pltpu.get_barrier_semaphore()
    for there in (to_x, to_y, to_sib):
        pl.semaphore_signal(barrier, inc=1, device_id=there, device_id_type=MESH)

    @pl.when(z < 3)
    def _():
        pl.semaphore_signal(barrier, inc=1, device_id=to_up, device_id_type=MESH)

    @pl.when(z > 0)
    def _():
        pl.semaphore_signal(barrier, inc=1, device_id=to_down, device_id_type=MESH)

    pl.semaphore_wait(barrier, 4 + ((z + 1) // 2) % 2)

    def source(k):
        if isinstance(k, int):
            return (1 + z % 2, 2 - 2 * (z % 2) + z // 2, 3 * (1 - z // 2))[k]
        a, b, d = (k - 1) * (k - 2) // 2, k * (2 - k), k * (k - 1) // 2
        return a * (1 + z % 2) + b * (2 - 2 * (z % 2) + z // 2) + d * (3 * (1 - z // 2))

    def region(p, zs, row, rows):
        at = pl.ds(pl.multiple_of(c * T + row, 64), rows)
        if isinstance(p, int) and p == 0:
            return gkv_ref.at[zs, at, :]
        return g_ref.at[p - 1, zs, at, :]

    def remote(src, dst, send, recv, there):
        return pltpu.make_async_remote_copy(src_ref=src, dst_ref=dst, send_sem=send, recv_sem=recv, device_id=there, device_id_type=MESH)

    def move(at, send, recv, there):
        return remote(at, at, send, recv, there)

    def z_copy(p, zs, i, there, quarter):
        return move(region(p, zs, quarter * QUARTER, QUARTER), sz.at[i], rz.at[p, zs], there)

    def x_copy(p, zs, i, quarter):
        return move(region(p, zs, quarter * QUARTER, QUARTER), sx.at[i], rx.at[p, zs], to_x)

    def y_copy(p, zs, i, quarter):
        return move(region(p, zs, quarter * QUARTER, QUARTER), sy.at[i], ry.at[p, zs], to_y)

    def dy_copy(p, zs, i, quarter):
        return move(region(p, zs, quarter * QUARTER, QUARTER // 2), sdy.at[i], rdy.at[p, zs], to_y)

    def dx_copy(p, zs, i, quarter):
        return move(region(p, zs, quarter * QUARTER + QUARTER // 2, QUARTER // 2), sdx.at[i], rdx.at[p, zs], to_x)

    def s_copy(p, zs, i):
        return move(region(p, zs, 0, T), ss.at[i], rs.at[p, zs], to_sib)

    def z_arrives(p, k, i):
        zs = source(k)
        z_copy(p, zs, i, to_sib, dp).wait_recv()

        @pl.when((zs < z) & (z < 3))
        def _():
            z_copy(p, zs, i, to_up, dp).start()

        @pl.when((zs > z) & (z > 0))
        def _():
            z_copy(p, zs, i, to_down, dp).start()

        x_copy(p, zs, i, dp).start()
        y_copy(p, zs, i, dp).start()

    def xy_arrive(p, k, i):
        zs = source(k)
        x_copy(p, zs, i, dpx).wait_recv()
        dy_copy(p, zs, i, dpx).start()
        y_copy(p, zs, i, dpy).wait_recv()
        dx_copy(p, zs, i, dpy).start()

    def d_arrive(p, k, i):
        zs = source(k)
        dy_copy(p, zs, i, dpd).wait_recv()
        dx_copy(p, zs, i, dpd).wait_recv()
        s_copy(p, zs, i).start()

    def sent(p, k, i):
        zs = source(k)

        @pl.when(((zs < z) & (z < 3)) | ((zs > z) & (z > 0)))
        def _():
            z_copy(p, zs, i, to_sib, dp).wait_send()

        x_copy(p, zs, i, dp).wait_send()
        y_copy(p, zs, i, dp).wait_send()
        dy_copy(p, zs, i, dpx).wait_send()
        dx_copy(p, zs, i, dpy).wait_send()
        s_copy(p, zs, i).wait_send()

    def own(p, rows):
        if p == 0:
            return wkv_ref.at[rows, :]
        return (wq_ref if p < 3 else wo_ref).at[rows, pl.ds((p - 1) % 2 * HALF, HALF)]

    def own_copies(p):
        mine = pl.ds(pl.multiple_of(dp * QUARTER, QUARTER), QUARTER)
        there = region(p, z, dp * QUARTER, QUARTER)
        return (remote(own(p, mine), there, sup.at[p], rz.at[p, z], to_up), remote(own(p, mine), there, sdown.at[p], rz.at[p, z], to_down),
                remote(own(p, pl.ds(0, T)), region(p, z, 0, T), sown.at[p], rs.at[p, z], to_sib))

    def issue_own(p, act):
        up, down, across = own_copies(p)
        pl.when(z < 3)(lambda: act(up))
        pl.when(z > 0)(lambda: act(down))
        act(across)

    start, finish = lambda copy: copy.start(), lambda copy: copy.wait_send()
    issue_own(0, start)
    loads = [pltpu.make_async_copy(x_ref, x_s, small_sem.at[0])]
    for copy in loads:
        copy.start()
    issue_own(1, start)
    for copy in loads:
        copy.wait()

    def norm(i, _):
        rows = pl.ds(pl.multiple_of(i * 16, 16), 16)
        wide = x_s[rows, :].astype(F32)
        scale = lax.rsqrt(jnp.mean(wide * wide, -1, keepdims=True) + 1e-6)
        lhs_s[0, rows, :] = (wide * scale * gain_ref[...].astype(F32)).astype(BF16)

    lax.fori_loop(0, T // 16, norm, None)

    def load_other(p, zs):
        rows = 2 * T
        if isinstance(p, int) and p == 0:
            return pltpu.make_async_copy(gkv_ref.at[zs], w_s.at[:, pl.ds(0, 1024)], load_sem.at[0])
        return pltpu.make_async_copy(g_ref.at[p - 1, zs], w_s, load_sem.at[0])

    def load_own(p):
        mine, other = pl.ds(pl.multiple_of(c * T, T), T), pl.ds(pl.multiple_of((1 - c) * T, T), T)
        wide = 1024 if p == 0 else HALF
        there = gkv_ref.at[z] if p == 0 else g_ref.at[p - 1, z]
        return (pltpu.make_async_copy(own(p, pl.ds(0, T)), w_s.at[mine, pl.ds(0, wide)], load_sem.at[0]),
                pltpu.make_async_copy(there.at[other, :], w_s.at[other, pl.ds(0, wide)], load_sem.at[1]))

    def sibling_arrived(p, zs):
        other = pl.ds(pl.multiple_of((1 - c) * T, T), T)
        there = gkv_ref.at[zs, other, :] if isinstance(p, int) and p == 0 else g_ref.at[p - 1, zs, other, :]
        remote(there, there, sown.at[0], rs.at[p, zs], to_sib).wait_recv()

    def multiply(which, zs, wide):
        deep = pl.ds(pl.multiple_of(zs * 1024, 1024), 1024)

        def tile(j, _):
            at = pl.ds(pl.multiple_of(j * 256, 256), 256)
            acc_s[:, at] += jnp.dot(lhs_s[which, :, deep], w_s[:, at], preferred_element_type=F32)

        lax.fori_loop(0, wide // 256, tile, None)

    def turned(t):
        t = t.astype(BF16).astype(F32)
        return (t * cos_ref[...] + pltpu.roll(t, HEAD // 2, 1) * sin_ref[...]).astype(BF16)

    def project_kv():
        sibling_arrived(0, z)
        for copy in load_own(0):
            copy.start()
        acc_s[:, :1024] = jnp.zeros((T, 1024), F32)
        for copy in load_own(0):
            copy.wait()
        multiply(0, z, 1024)

        def rest(k, _):
            zs = source(k)
            sibling_arrived(0, zs)
            load_other(0, zs).start()
            load_other(0, zs).wait()
            multiply(0, zs, 1024)

        lax.fori_loop(0, 3, rest, None)
        for h in range(4):
            kv_s[sp, h] = turned(acc_s[:, h * HEAD : (h + 1) * HEAD])
            kv_s[sp, 4 + h] = acc_s[:, 512 + h * HEAD : 512 + (h + 1) * HEAD].astype(BF16)

    def kv_up(j, src, sem):
        return remote(kv_s.at[src], kv_s.at[src], sem, rkv.at[src // 2], to_up)

    def kv_across(src, sem):
        return remote(kv_s.at[src], kv_s.at[src], sem, rskv.at[src // 2], to_sib)

    def kv_arrives(j, wait_only=False):
        @pl.when(z >= j)
        def _():
            src = sp - 2 * j
            if not wait_only:
                kv_up(j, src, skv_up.at[j]).wait_recv()

            @pl.when(z < 3)
            def _():
                copy = kv_up(j, src, skv_up.at[j])
                copy.wait_send() if wait_only else copy.start()

            copy = kv_across(src, skv_sib.at[j])
            copy.wait_send() if wait_only else copy.start()

    def kv_from_sibling():
        for j in range(4):
            @pl.when(z >= j)
            def _():
                src = (z - j) * 2 + (1 - c)
                kv_across(src, skv_sib.at[j]).wait_recv()

    e = HEAD**-0.5 * LOG2E

    def attend(h, j, masked):
        keys, values = kv_s[j, h], kv_s[j, 4 + h]
        scores = [_dot(keys, q_s[h * 8 + n], 1, 1) for n in range(8)]
        if masked:
            ok = lax.broadcasted_iota(jnp.int32, (T, T), 1) >= lax.broadcasted_iota(jnp.int32, (T, T), 0)
        weights, keeps = [], []
        for n, s in enumerate(scores):
            if masked:
                s = jnp.where(ok, s, HIDDEN)
            old = top_s[n : n + 1, :]
            top = jnp.maximum(old, s.max(axis=0, keepdims=True))
            top_s[n : n + 1, :] = top
            weights.append(jnp.exp2((s - top) * e).astype(BF16))
            keeps.append(jnp.exp2((old - top) * e))
        values = jnp.concatenate([values.T, jnp.ones((8, T), BF16)], axis=0)
        for n, (p, keep) in enumerate(zip(weights, keeps)):
            mix_s[n] = mix_s[n] * keep + _dot(values, p, 1, 0)

    def attention(first, i, _):
        h, j = first + i // (sp + 1), i % (sp + 1)

        @pl.when(j == 0)
        def _():
            top_s[...] = jnp.full((8, T), NEG, F32)
            mix_s[...] = jnp.zeros((8, HEAD + 8, T), F32)

        pl.when(j < sp)(lambda: attend(h, j, False))

        @pl.when(j == sp)
        def _():
            attend(h, j, True)
            for n in range(8):
                at = pl.ds(pl.multiple_of(h * 1024 + n * HEAD, HEAD), HEAD)
                lhs_s[1, :, at] = (mix_s[n, :HEAD, :] * (1 / mix_s[n, HEAD : HEAD + 1, :])).T.astype(BF16)

    def finish_q(half):
        def head(n, _):
            q_s[half * 16 + n] = turned(acc_s[:, pl.ds(pl.multiple_of(n * HEAD, HEAD), HEAD)])

        lax.fori_loop(0, 16, head, None)

    def y_copy_out(half):
        at = pl.ds(pl.multiple_of(half * HALF, HALF), HALF)
        return pltpu.make_async_copy(x_s.at[:, at], y_ref.at[:, at], y_sem.at[half])

    def finish_y(half):
        def tile(n, _):
            at = pl.ds(pl.multiple_of(half * HALF + n * 256, 256), 256)
            x_s[:, at] = (x_s[:, at].astype(F32) + acc_s[:, pl.ds(pl.multiple_of(n * 256, 256), 256)]).astype(BF16)

        lax.fori_loop(0, HALF // 256, tile, None)
        y_copy_out(half).start()

    def consume(i, _):
        p, k = i // 3 + 1, i % 3
        which = (p - 1) // 2

        @pl.when(k == 0)
        def _():
            sibling_arrived(p, z)
            for n in range(1, 5):
                @pl.when(p == n)
                def _():
                    for copy in load_own(n):
                        copy.start()
            acc_s[...] = jnp.zeros((T, HALF), F32)
            for copy in load_own(1):
                copy.wait()
            multiply(which, z, HALF)

        zs = source(k)
        sibling_arrived(p, zs)
        load_other(p, zs).start()
        load_other(p, zs).wait()
        multiply(which, zs, HALF)

        @pl.when(k == 2)
        def _():
            half = (p - 1) % 2
            pl.when(p < 3)(lambda: finish_q(half))
            pl.when(p >= 3)(lambda: finish_y(half))

    z_arrives(0, 0, 0)
    for k in range(3):
        z_arrives(0, k + 1, k + 1) if k < 2 else z_arrives(1, 0, 3)
        xy_arrive(0, k, k)
        if k:
            d_arrive(0, k - 1, k - 1)

    def step(t, _):
        u, r = t // 3, t % 3

        @pl.when(r == 0)
        def _():
            for n in range(3):
                pl.when(u == 3 * n)(lambda: issue_own(n + 2, start))

            @pl.when(u + 1 < SLOTS)
            def _():
                v = u + 1
                z_arrives(v // 3 + 1, v % 3, v + 3)

        @pl.when((r == 1) & (u < SLOTS))
        def _():
            xy_arrive(u // 3 + 1, u % 3, u + 3)

        @pl.when(r == 2)
        def _():
            pl.when(u == 0)(lambda: d_arrive(0, 2, 2))

            @pl.when((u >= 1) & (u <= SLOTS))
            def _():
                v = u - 1
                d_arrive(v // 3 + 1, v % 3, v + 3)

            @pl.when(u == 1)
            def _():
                project_kv()
                pl.when(z < 3)(lambda: kv_up(0, sp, skv_own.at[0]).start())
                kv_across(sp, skv_own.at[1]).start()

            for j in range(1, 4):
                pl.when(u == j + 1)(lambda: kv_arrives(j))
            lo = jnp.where(u < 8, jnp.maximum(u - 2, 0), jnp.where(u < 12, 6, u - 2))
            hi = jnp.where(u < 8, jnp.maximum(u - 1, 0), jnp.where(u < 11, 6, u - 1))
            lax.fori_loop(lo, hi, consume, None)
            pl.when(u == 4)(kv_from_sibling)

        late = t >= 23
        j, parts = jnp.where(late, t - 23, t - 14), jnp.where(late, 12, 9)
        n = 2 * (sp + 1)
        busy = (t >= 14) & (t < 35)
        lo, hi = jnp.where(busy, n * j // parts, 0), jnp.where(busy, n * (j + 1) // parts, 0)
        lax.fori_loop(lo, hi, functools.partial(attention, jnp.where(late, 2, 0)), None)

    lax.fori_loop(0, 3 * (SLOTS + 2), step, None)

    for p in range(5):
        issue_own(p, finish)
    for k in range(3):
        sent(0, k, k)
    lax.fori_loop(0, SLOTS, lambda v, _: sent(v // 3 + 1, v % 3, v + 3), None)
    pl.when(z < 3)(lambda: kv_up(0, sp, skv_own.at[0]).wait_send())
    kv_across(sp, skv_own.at[1]).wait_send()
    for j in range(1, 4):
        kv_arrives(j, True)
    for half in range(2):
        y_copy_out(half).wait()


def solution(mesh):
    dma = pltpu.SemaphoreType.DMA

    def step(x, gain, wq, wk, wv, wo):
        place = lax.axis_index("sp") * T + jnp.arange(T)
        half = HEAD // 2
        angle = place.astype(F32)[:, None] * THETA ** (-jnp.arange(half, dtype=F32) / half)
        cos, sin = jnp.cos(angle), jnp.sin(angle)
        cos, sin = jnp.concatenate([cos, cos], 1), jnp.concatenate([-sin, sin], 1)
        hbm, vmem = pl.BlockSpec(memory_space=pl.ANY), pl.BlockSpec(memory_space=pltpu.VMEM)
        y, _, _ = pl.pallas_call(
            _kernel,
            in_specs=[hbm, vmem, hbm, hbm, hbm, vmem, vmem],
            out_specs=[hbm, hbm, hbm],
            out_shape=[jax.ShapeDtypeStruct((T, D), BF16), jax.ShapeDtypeStruct((4, 1024, 1024), BF16),
                       jax.ShapeDtypeStruct((4, 4, 1024, HALF), BF16)],
            scratch_shapes=[
                pltpu.VMEM((T, D), BF16), pltpu.VMEM((2, T, D), BF16), pltpu.VMEM((32, T, HEAD), BF16), pltpu.VMEM((8, 8, T, HEAD), BF16),
                pltpu.VMEM((T, HALF), F32), pltpu.VMEM((1024, HALF), BF16), pltpu.VMEM((8, HEAD + 8, T), F32), pltpu.VMEM((8, T), F32),
                *[dma((5, 4))] * 6, *[dma((15,))] * 6, *[dma((5,))] * 3,
                dma((4,)), dma((4,)), dma((4,)), dma((4,)), dma((2,)), dma((2,)), dma((1,)), dma((2,)),
            ],
            compiler_params=pltpu.CompilerParams(collective_id=0, has_side_effects=True, vmem_limit_bytes=VMEM),
            cost_estimate=pl.CostEstimate(flops=2 * T * D * (2 * D + 1024) + 4 * T * D * D, transcendentals=32 * T * D, bytes_accessed=2**28),
        )(x, gain[None], jnp.concatenate([wk, wv], 1), wq, wo, cos, sin)
        return y

    tokens, whole = P(("dp", "sp"), None), P("sp", None)
    return jax.shard_map(
        step,
        mesh=mesh,
        in_specs=(tokens, P(None), whole, whole, whole, whole),
        out_specs=tokens,
        check_vma=False,
    )
```

```python
import functools

import jax
import jax.numpy as jnp
from jax import lax
from jax.experimental import pallas as pl
from jax.experimental.pallas import tpu as pltpu
from jax.sharding import PartitionSpec as P

MESH = pl.DeviceIdType.MESH
NEG = -1e30
HIDDEN = 2 * NEG
LOG2E = 1.4426950408889634
VMEM = 63 * 2**20
HEAD = 128
THETA = 10000
T = 512
D = 4096
WIDE = 1024
PHASES = 9
SLOTS = 3 * PHASES
QUARTER = T // 4
F32 = jnp.float32
BF16 = jnp.bfloat16

OWN, Z_IN, XY_OUT, XY_IN, D_IN, TAKE, KV_OUT, KV_IN, ATTEND, NORM = range(1, 11)
ORDERS = (
    (
        0x4326a11, 0x4126532, 0x4265332, 0x5324123, 0x3245766, 0x3247126, 0x6523465, 0x3521246, 0x3245969, 0x4665346,
        0x6935212, 0x6372459, 0x2466534, 0x9693521, 0x3463245, 0x4662125, 0x4972653, 0x5634593, 0x5346226, 0x4653462,
        0x3462653, 0x4653465, 0x6546653, 0x65654, 0x0, 0x0, 0x0, 0x0, 0x0,
    ),
    (
        0x3226a11, 0x3221243, 0x2346534, 0x3462251, 0x2457665, 0x4623271, 0x2348653, 0x4662521, 0x3495983, 0x6349596,
        0x6722125, 0x4693456, 0x3469593, 0x6221259, 0x6958634, 0x4695934, 0x5372212, 0x9563469, 0x4656349, 0x9822253,
        0x6663459, 0x5346534, 0x6534662, 0x5346534, 0x5465466, 0x656, 0x0, 0x0, 0x0,
    ),
    (
        0x3226a11, 0x3221243, 0x2346534, 0x3462251, 0x2457665, 0x4623271, 0x5346583, 0x2593466, 0x4889221, 0x3469563,
        0x6921259, 0x4956348, 0x1256372, 0x9348692, 0x5634695, 0x1263249, 0x3486925, 0x6346959, 0x7245995, 0x4993822,
        0x9349953, 0x5983495, 0x3459922, 0x5634666, 0x5634666, 0x6653466, 0x5654654, 0x6, 0x0,
    ),
    (
        0x4326a11, 0x4126532, 0x4265332, 0x5324123, 0x3245766, 0x2653486, 0x6534271, 0x9259346, 0x6958634, 0x3251249,
        0x2563469, 0x9348869, 0x2564895, 0x3469321, 0x4672956, 0x4895893, 0x3212596, 0x9656349, 0x9589324, 0x3212594,
        0x2959349, 0x9583497, 0x2259489, 0x2593493, 0x9345989, 0x3259498, 0x6656646, 0x5665646, 0x666666,
    ),
)


def _dot(a, b, ca, cb):
    return lax.dot_general(a, b, (((ca,), (cb,)), ((), ())), preferred_element_type=F32)


def _kernel(x_ref, gain_ref, wk_ref, wv_ref, wq_ref, wo_ref, turn_ref, y_ref, g_ref,
            x_s, lhs_s, q_s, kv_s, acc_s, w_s, mix_s, top_s, cos_s, sin_s,
            rz, rx, ry, rdx, rdy, rs, sz, sx, sy, sdx, sdy, ss, sup, sdown, sown,
            rkv, rskv, skv_up, skv_sib, load_sem, x_sem, y_sem):
    dp, sp = lax.axis_index("dp"), lax.axis_index("sp")
    xq, yq = dp // 2, dp % 2
    z, c = sp // 2, sp % 2
    dpx, dpy = (1 - xq) * 2 + yq, xq * 2 + (1 - yq)
    dpd = 3 - dp
    to_x, to_y, to_sib = (dpx, sp), (dpy, sp), (dp, z * 2 + (1 - c))
    to_up, to_down = (dp, sp + 2), (dp, sp - 2)

    x_load = pltpu.make_async_copy(x_ref, x_s, x_sem.at[0])
    x_load.start()
    barrier = pltpu.get_barrier_semaphore()
    for there in (to_x, to_y, to_sib):
        pl.semaphore_signal(barrier, inc=1, device_id=there, device_id_type=MESH)

    @pl.when(z < 3)
    def _():
        pl.semaphore_signal(barrier, inc=1, device_id=to_up, device_id_type=MESH)

    @pl.when(z > 0)
    def _():
        pl.semaphore_signal(barrier, inc=1, device_id=to_down, device_id_type=MESH)

    pl.semaphore_wait(barrier, 4 + ((z + 1) // 2) % 2)

    def source(k):
        a, b, d = (k - 1) * (k - 2) // 2, k * (2 - k), k * (k - 1) // 2
        return a * (1 + z % 2) + b * (2 - 2 * (z % 2) + z // 2) + d * (3 * (1 - z // 2))

    def region(p, zs, row, rows):
        return g_ref.at[p, zs, pl.ds(pl.multiple_of(c * T + row, 64), rows), :]

    def remote(src, dst, send, recv, there):
        return pltpu.make_async_remote_copy(src_ref=src, dst_ref=dst, send_sem=send, recv_sem=recv, device_id=there, device_id_type=MESH)

    def move(at, send, recv, there):
        return remote(at, at, send, recv, there)

    def z_copy(p, zs, i, there, quarter):
        return move(region(p, zs, quarter * QUARTER, QUARTER), sz.at[i], rz.at[p, zs], there)

    def x_copy(p, zs, i, quarter):
        return move(region(p, zs, quarter * QUARTER, QUARTER), sx.at[i], rx.at[p, zs], to_x)

    def y_copy(p, zs, i, quarter):
        return move(region(p, zs, quarter * QUARTER, QUARTER), sy.at[i], ry.at[p, zs], to_y)

    def dy_copy(p, zs, i, quarter):
        return move(region(p, zs, quarter * QUARTER, QUARTER // 2), sdy.at[i], rdy.at[p, zs], to_y)

    def dx_copy(p, zs, i, quarter):
        return move(region(p, zs, quarter * QUARTER + QUARTER // 2, QUARTER // 2), sdx.at[i], rdx.at[p, zs], to_x)

    def s_copy(p, zs, i):
        return move(region(p, zs, 0, T), ss.at[i], rs.at[p, zs], to_sib)

    def z_in(i):
        p, zs = i // 3, source(i % 3)
        z_copy(p, zs, i, to_sib, dp).wait_recv()

        @pl.when((zs < z) & (z < 3))
        def _():
            z_copy(p, zs, i, to_up, dp).start()

        @pl.when((zs > z) & (z > 0))
        def _():
            z_copy(p, zs, i, to_down, dp).start()

    def xy_out(i):
        p, zs = i // 3, source(i % 3)
        x_copy(p, zs, i, dp).start()
        y_copy(p, zs, i, dp).start()

    def xy_in(i):
        p, zs = i // 3, source(i % 3)
        x_copy(p, zs, i, dpx).wait_recv()
        dy_copy(p, zs, i, dpx).start()
        y_copy(p, zs, i, dpy).wait_recv()
        dx_copy(p, zs, i, dpy).start()

    def d_in(i):
        p, zs = i // 3, source(i % 3)
        dy_copy(p, zs, i, dpd).wait_recv()
        dx_copy(p, zs, i, dpd).wait_recv()
        s_copy(p, zs, i).start()

    def sent(i, _):
        p, zs = i // 3, source(i % 3)

        @pl.when(((zs < z) & (z < 3)) | ((zs > z) & (z > 0)))
        def _():
            z_copy(p, zs, i, to_sib, dp).wait_send()

        x_copy(p, zs, i, dp).wait_send()
        y_copy(p, zs, i, dp).wait_send()
        dy_copy(p, zs, i, dpx).wait_send()
        dx_copy(p, zs, i, dpy).wait_send()
        s_copy(p, zs, i).wait_send()

    def own_parts(p, act):
        @pl.when(p == 0)
        def _():
            act(wk_ref, 0, WIDE // 2, 0)
            act(wv_ref, 0, WIDE // 2, WIDE // 2)

        pl.when((p > 0) & (p < 5))(lambda: act(wq_ref, pl.multiple_of((p - 1) * WIDE, WIDE), WIDE, 0))
        pl.when(p >= 5)(lambda: act(wo_ref, pl.multiple_of((p - 5) * WIDE, WIDE), WIDE, 0))

    def send_own(p):
        mine = pl.ds(pl.multiple_of(dp * QUARTER, QUARTER), QUARTER)
        here = pl.ds(pl.multiple_of(c * T + dp * QUARTER, QUARTER), QUARTER)
        shard = pl.ds(pl.multiple_of(c * T, T), T)

        def act(ref, at, wide, to):
            src, dst = pl.ds(at, wide), pl.ds(to, wide)
            part, there = ref.at[mine, src], g_ref.at[p, z, here, dst]
            pl.when(z < 3)(lambda: remote(part, there, sup.at[p], rz.at[p, z], to_up).start())
            pl.when(z > 0)(lambda: remote(part, there, sdown.at[p], rz.at[p, z], to_down).start())
            remote(ref.at[:, src], g_ref.at[p, z, shard, dst], sown.at[p], rs.at[p, z], to_sib).start()

        own_parts(p, act)

    def own_sent(p, _):
        part = region(p, z, dp * QUARTER, QUARTER)
        pl.when(z < 3)(lambda: move(part, sup.at[p], rz.at[p, z], to_up).wait_send())
        pl.when(z > 0)(lambda: move(part, sdown.at[p], rz.at[p, z], to_down).wait_send())
        move(region(p, z, 0, T), sown.at[p], rs.at[p, z], to_sib).wait_send()

    def norm():
        x_load.wait()
        lane = lax.broadcasted_iota(jnp.int32, (T, HEAD), 1) < HEAD // 2
        table = turn_ref[...]
        other = pltpu.roll(table, HEAD // 2, 1)
        cos_s[...] = jnp.where(lane, table, other)
        sin_s[...] = jnp.where(lane, -other, table)

        def rows(i, _):
            at = pl.ds(pl.multiple_of(i * 16, 16), 16)
            wide = x_s[at, :].astype(F32)
            scale = lax.rsqrt(jnp.mean(wide * wide, -1, keepdims=True) + 1e-6)
            lhs_s[0, at, :] = (wide * scale * gain_ref[...].astype(F32)).astype(BF16)

        lax.fori_loop(0, T // 16, rows, None)

    def unit_source(m):
        return jnp.where(m == 0, z, source(m - 1))

    def load_unit(i):
        p, m, at = i // 4, i % 4, i % 2
        zs = unit_source(m)
        mine, other = pl.ds(pl.multiple_of(c * T, T), T), pl.ds(pl.multiple_of((1 - c) * T, T), T)
        there = g_ref.at[p, zs, other, :]
        remote(there, there, sown.at[0], rs.at[p, zs], to_sib).wait_recv()

        @pl.when(m == 0)
        def _():
            pltpu.make_async_copy(there, w_s.at[at, other, :], load_sem.at[at]).start()
            own_parts(p, lambda ref, start, wide, to: pltpu.make_async_copy(
                ref.at[:, pl.ds(start, wide)], w_s.at[at, mine, pl.ds(to, wide)], load_sem.at[at]).start())

        pl.when(m > 0)(lambda: pltpu.make_async_copy(g_ref.at[p, zs], w_s.at[at], load_sem.at[at]).start())

    def turned(t):
        t = t.astype(BF16).astype(F32)
        return (t * cos_s[...] + pltpu.roll(t, HEAD // 2, 1) * sin_s[...]).astype(BF16)

    def y_out(p):
        at = pl.ds(pl.multiple_of((p - 5) * WIDE, WIDE), WIDE)
        return pltpu.make_async_copy(x_s.at[:, at], y_ref.at[:, at], y_sem.at[p - 5])

    def work_unit(i):
        p, m, at = i // 4, i % 4, i % 2
        zs = unit_source(m)
        which = jnp.where(p < 5, 0, 1)
        pltpu.make_async_copy(g_ref.at[p, zs], w_s.at[at], load_sem.at[at]).wait()

        @pl.when(m == 0)
        def _():
            acc_s[...] = jnp.zeros((T, WIDE), F32)

        deep = pl.ds(pl.multiple_of(zs * WIDE, WIDE), WIDE)

        def tile(j, _):
            cols = pl.ds(pl.multiple_of(j * 256, 256), 256)
            acc_s[:, cols] += jnp.dot(lhs_s[which, :, deep], w_s[at, :, cols], preferred_element_type=F32)

        lax.fori_loop(0, WIDE // 256, tile, None)

        @pl.when((m == 3) & (p == 0))
        def _():
            for h in range(4):
                kv_s[sp, h, 0] = turned(acc_s[:, h * HEAD : (h + 1) * HEAD])
                kv_s[sp, h, 1] = acc_s[:, 512 + h * HEAD : 512 + (h + 1) * HEAD].astype(BF16)

        @pl.when((m == 3) & (p > 0) & (p < 5))
        def _():
            def head(n, _):
                q_s[(p - 1) * 8 + n] = turned(acc_s[:, pl.ds(pl.multiple_of(n * HEAD, HEAD), HEAD)])

            lax.fori_loop(0, 8, head, None)

        @pl.when((m == 3) & (p >= 5))
        def _():
            def part(n, _):
                cols = pl.ds(pl.multiple_of((p - 5) * WIDE + n * 256, 256), 256)
                x_s[:, cols] = (x_s[:, cols].astype(F32) + acc_s[:, pl.ds(pl.multiple_of(n * 256, 256), 256)]).astype(BF16)

            lax.fori_loop(0, WIDE // 256, part, None)
            y_out(p).start()

    def take(i):
        load_unit(i)
        pl.when(i > 0)(lambda: work_unit(i - 1))

    def kv_up(src, h, j):
        return move(kv_s.at[src, h], skv_up.at[j, h], rkv.at[src // 2, h], to_up)

    def kv_across(src, h, j):
        return move(kv_s.at[src, h], skv_sib.at[j, h], rskv.at[src // 2, h], to_sib)

    def kv_out(h):
        pl.when(z < 3)(lambda: kv_up(sp, h, 0).start())
        kv_across(sp, h, 0).start()

    def kv_in(i):
        chips = jnp.maximum(z, 1)
        h, j = i // chips, 1 + i % chips
        src = sp - 2 * j
        kv_up(src, h, j).wait_recv()
        pl.when(z < 3)(lambda: kv_up(src, h, j).start())
        kv_across(src, h, j).start()

    e = HEAD**-0.5 * LOG2E

    def block(h, src, masked):
        keys, values = kv_s[src, h, 0], kv_s[src, h, 1]
        scores = [_dot(keys, q_s[h * 8 + n], 1, 1) for n in range(8)]
        if masked:
            ok = lax.broadcasted_iota(jnp.int32, (T, T), 1) >= lax.broadcasted_iota(jnp.int32, (T, T), 0)
        weights, keeps = [], []
        for n, s in enumerate(scores):
            if masked:
                s = jnp.where(ok, s, HIDDEN)
            old = top_s[n : n + 1, :]
            top = jnp.maximum(old, s.max(axis=0, keepdims=True))
            top_s[n : n + 1, :] = top
            weights.append(jnp.exp2((s - top) * e).astype(BF16))
            keeps.append(jnp.exp2((old - top) * e))
        values = jnp.concatenate([values.T, jnp.ones((8, T), BF16)], axis=0)
        for n, (p, keep) in enumerate(zip(weights, keeps)):
            mix_s[n] = mix_s[n] * keep + _dot(values, p, 1, 0)

    def attend(i):
        blocks = 2 * z + 2
        h, j = i // blocks, i % blocks
        odd = j % 2
        src = 2 * (z - j // 2) + jnp.where(odd == 0, c, 1 - c)

        @pl.when(odd == 1)
        def _():
            kv_across(src, h, 0).wait_recv()

        @pl.when(j == 0)
        def _():
            top_s[...] = jnp.full((8, T), NEG, F32)
            mix_s[...] = jnp.zeros((8, HEAD + 8, T), F32)
            block(h, src, True)

        pl.when((j > 0) & (src < sp))(lambda: block(h, src, False))

        @pl.when(j == blocks - 1)
        def _():
            for n in range(8):
                at = pl.ds(pl.multiple_of(h * WIDE + n * HEAD, HEAD), HEAD)
                lhs_s[1, :, at] = (mix_s[n, :HEAD, :] * (1 / mix_s[n, HEAD : HEAD + 1, :])).T.astype(BF16)

    handlers = ((OWN, send_own), (Z_IN, z_in), (XY_OUT, xy_out), (XY_IN, xy_in), (D_IN, d_in), (TAKE, take), (KV_OUT, kv_out), (KV_IN, kv_in),
                (ATTEND, attend), (NORM, lambda i: norm()))

    def seven(g, counts):
        at, word = z * len(ORDERS[0]) + g, jnp.int32(0)
        for n, number in enumerate(sum(ORDERS, ())):
            word = jnp.where(at == n, number, word)

        def one(_, state):
            word, counts = state[0], state[1:]
            op = word % 16
            for (code, handler), count in zip(handlers, counts):
                pl.when(op == code)(functools.partial(handler, count))
            return (word // 16, *(count + jnp.where(op == code, 1, 0) for (code, _), count in zip(handlers, counts)))

        return lax.fori_loop(0, 7, one, (word, *counts))[1:]

    lax.fori_loop(0, len(ORDERS[0]), seven, (jnp.int32(0),) * len(handlers))
    work_unit(jnp.int32(4 * PHASES - 1))

    lax.fori_loop(0, PHASES, own_sent, None)
    lax.fori_loop(0, SLOTS, sent, None)

    def kv_sent(h, _):
        for j in range(4):
            @pl.when(z >= j)
            def _():
                pl.when(z < 3)(lambda: kv_up(sp - 2 * j, h, j).wait_send())
                kv_across(sp - 2 * j, h, j).wait_send()

    lax.fori_loop(0, 4, kv_sent, None)
    for p in range(5, PHASES):
        y_out(p).wait()


def solution(mesh):
    dma = pltpu.SemaphoreType.DMA

    def step(x, gain, wq, wk, wv, wo):
        place = lax.axis_index("sp") * T + jnp.arange(T)
        half = HEAD // 2
        angle = place.astype(F32)[:, None] * THETA ** (-jnp.arange(half, dtype=F32) / half)
        turn = jnp.concatenate([jnp.cos(angle), jnp.sin(angle)], 1)
        hbm, vmem = pl.BlockSpec(memory_space=pl.ANY), pl.BlockSpec(memory_space=pltpu.VMEM)
        y, _ = pl.pallas_call(
            _kernel,
            in_specs=[hbm, vmem, hbm, hbm, hbm, hbm, vmem],
            out_specs=[hbm, hbm],
            out_shape=[jax.ShapeDtypeStruct((T, D), BF16), jax.ShapeDtypeStruct((PHASES, 4, 2 * T, WIDE), BF16)],
            scratch_shapes=[
                pltpu.VMEM((T, D), BF16), pltpu.VMEM((2, T, D), BF16), pltpu.VMEM((32, T, HEAD), BF16), pltpu.VMEM((8, 4, 2, T, HEAD), BF16),
                pltpu.VMEM((T, WIDE), F32), pltpu.VMEM((2, 2 * T, WIDE), BF16), pltpu.VMEM((8, HEAD + 8, T), F32), pltpu.VMEM((8, T), F32),
                pltpu.VMEM((T, HEAD), F32), pltpu.VMEM((T, HEAD), F32),
                *[dma((PHASES, 4))] * 6, *[dma((SLOTS,))] * 6, *[dma((PHASES,))] * 3,
                dma((4, 4)), dma((4, 4)), dma((4, 4)), dma((4, 4)), dma((2,)), dma((1,)), dma((4,)),
            ],
            compiler_params=pltpu.CompilerParams(collective_id=0, has_side_effects=True, vmem_limit_bytes=VMEM),
            cost_estimate=pl.CostEstimate(flops=2 * T * D * (2 * D + 1024) + 4 * T * D * D, transcendentals=32 * T * D, bytes_accessed=2**28),
        )(x, gain, wk, wv, wq, wo, turn)
        return y

    tokens, whole = P(("dp", "sp"), None), P("sp", None)
    return jax.shard_map(
        step,
        mesh=mesh,
        in_specs=(tokens, P(None), whole, whole, whole, whole),
        out_specs=tokens,
        check_vma=False,
    )
```

```python
import functools

import jax
import jax.numpy as jnp
from jax import lax
from jax.experimental import pallas as pl
from jax.experimental.pallas import tpu as pltpu
from jax.sharding import PartitionSpec as P

MESH = pl.DeviceIdType.MESH
NEG = -1e30
HIDDEN = 2 * NEG
LOG2E = 1.4426950408889634
VMEM = 56 * 2**20
HEAD = 128
THETA = 10000
T = 512
D = 4096
WIDE = 1024
PHASES = 9
SLOTS = 3 * PHASES
QUARTER = T // 4
F32 = jnp.float32
BF16 = jnp.bfloat16

OWN, Z_IN, XY_OUT, XY_IN, D_IN, TAKE, KV_OUT, KV_IN, ATTEND, NORM = range(1, 11)
ORDERS = (
    (
        0x4326a11, 0x4126532, 0x3265332, 0x3324124, 0x6653254, 0x3321247, 0x6372546, 0x6325124, 0x4599346, 0x4621232,
        0x3472653, 0x5934665, 0x2125649, 0x6653463, 0x4959324, 0x3725126, 0x6625346, 0x6495934, 0x3322465, 0x5346265,
        0x2656546, 0x4654643, 0x6565465, 0x66565, 0x0, 0x0, 0x0, 0x0, 0x0,
    ),
    (
        0x3226a11, 0x3221243, 0x2465433, 0x3423321, 0x2125654, 0x7247663, 0x1265343, 0x4685342, 0x4686532, 0x7253212,
        0x5934969, 0x6656349, 0x6895934, 0x9322124, 0x6563495, 0x2959346, 0x6327241, 0x3549695, 0x9593466, 0x2259498,
        0x5634632, 0x4653466, 0x6543265, 0x6546546, 0x6565654, 0x665, 0x0, 0x0, 0x0,
    ),
    (
        0x3226a11, 0x3221243, 0x2465433, 0x3423321, 0x2125654, 0x7247663, 0x4865343, 0x6322125, 0x3466534, 0x4695889,
        0x9593212, 0x9593468, 0x3212724, 0x3468656, 0x4896959, 0x4626953, 0x9372512, 0x6934596, 0x6895934, 0x3222456,
        0x9593499, 0x9959348, 0x4229594, 0x6656633, 0x4665646, 0x5446565, 0x6565656, 0x6, 0x0,
    ),
    (
        0x4326a11, 0x4126532, 0x3265332, 0x3324124, 0x6653254, 0x3321247, 0x6372546, 0x9466584, 0x2959489, 0x9634321,
        0x6532595, 0x5648866, 0x1249689, 0x5949332, 0x6637259, 0x8949684, 0x2124695, 0x5595933, 0x8946326, 0x9498949,
        0x3372125, 0x2499595, 0x8948993, 0x2254995, 0x8532933, 0x6324949, 0x6656466, 0x6646665, 0x666565,
    ),
)


def _dot(a, b, ca, cb):
    return lax.dot_general(a, b, (((ca,), (cb,)), ((), ())), preferred_element_type=F32)


def _kernel(x_ref, gain_ref, wk_ref, wv_ref, wq_ref, wo_ref, turn_ref, y_ref, g_ref,
            x_s, lhs_s, q_s, kv_s, acc_s, w_s, mix_s, top_s, cos_s, sin_s,
            rz, rx, ry, rdx, rdy, rs, sz, sx, sy, sdx, sdy, ss, sup, sdown, sown,
            rkv, rskv, skv_up, skv_sib, load_sem, x_sem):
    dp, sp = lax.axis_index("dp"), lax.axis_index("sp")
    xq, yq = dp // 2, dp % 2
    z, c = sp // 2, sp % 2
    dpx, dpy = (1 - xq) * 2 + yq, xq * 2 + (1 - yq)
    dpd = 3 - dp
    to_x, to_y, to_sib = (dpx, sp), (dpy, sp), (dp, z * 2 + (1 - c))
    to_up, to_down = (dp, sp + 2), (dp, sp - 2)

    x_load = pltpu.make_async_copy(x_ref, x_s, x_sem.at[0])
    x_load.start()
    barrier = pltpu.get_barrier_semaphore()
    for there in (to_x, to_y, to_sib):
        pl.semaphore_signal(barrier, inc=1, device_id=there, device_id_type=MESH)

    @pl.when(z < 3)
    def _():
        pl.semaphore_signal(barrier, inc=1, device_id=to_up, device_id_type=MESH)

    @pl.when(z > 0)
    def _():
        pl.semaphore_signal(barrier, inc=1, device_id=to_down, device_id_type=MESH)

    pl.semaphore_wait(barrier, 4 + ((z + 1) // 2) % 2)

    def source(k):
        a, b, d = (k - 1) * (k - 2) // 2, k * (2 - k), k * (k - 1) // 2
        return a * (1 + z % 2) + b * (2 - 2 * (z % 2) + z // 2) + d * (3 * (1 - z // 2))

    def region(p, zs, row, rows):
        return g_ref.at[p, zs, pl.ds(pl.multiple_of(c * T + row, 64), rows), :]

    def remote(src, dst, send, recv, there):
        return pltpu.make_async_remote_copy(src_ref=src, dst_ref=dst, send_sem=send, recv_sem=recv, device_id=there, device_id_type=MESH)

    def move(at, send, recv, there):
        return remote(at, at, send, recv, there)

    def z_copy(p, zs, i, there, quarter):
        return move(region(p, zs, quarter * QUARTER, QUARTER), sz.at[i], rz.at[p, zs], there)

    def x_copy(p, zs, i, quarter):
        return move(region(p, zs, quarter * QUARTER, QUARTER), sx.at[i], rx.at[p, zs], to_x)

    def y_copy(p, zs, i, quarter):
        return move(region(p, zs, quarter * QUARTER, QUARTER), sy.at[i], ry.at[p, zs], to_y)

    def dy_copy(p, zs, i, quarter):
        return move(region(p, zs, quarter * QUARTER, QUARTER // 2), sdy.at[i], rdy.at[p, zs], to_y)

    def dx_copy(p, zs, i, quarter):
        return move(region(p, zs, quarter * QUARTER + QUARTER // 2, QUARTER // 2), sdx.at[i], rdx.at[p, zs], to_x)

    def s_copy(p, zs, i):
        return move(region(p, zs, 0, T), ss.at[i], rs.at[p, zs], to_sib)

    def z_in(i):
        p, zs = i // 3, source(i % 3)
        z_copy(p, zs, i, to_sib, dp).wait_recv()

        @pl.when((zs < z) & (z < 3))
        def _():
            z_copy(p, zs, i, to_up, dp).start()

        @pl.when((zs > z) & (z > 0))
        def _():
            z_copy(p, zs, i, to_down, dp).start()

    def xy_out(i):
        p, zs = i // 3, source(i % 3)
        x_copy(p, zs, i, dp).start()
        y_copy(p, zs, i, dp).start()

    def xy_in(i):
        p, zs = i // 3, source(i % 3)
        x_copy(p, zs, i, dpx).wait_recv()
        dy_copy(p, zs, i, dpx).start()
        y_copy(p, zs, i, dpy).wait_recv()
        dx_copy(p, zs, i, dpy).start()

    def d_in(i):
        p, zs = i // 3, source(i % 3)
        dy_copy(p, zs, i, dpd).wait_recv()
        dx_copy(p, zs, i, dpd).wait_recv()
        s_copy(p, zs, i).start()

    def sent(i, _):
        p, zs = i // 3, source(i % 3)

        @pl.when(((zs < z) & (z < 3)) | ((zs > z) & (z > 0)))
        def _():
            z_copy(p, zs, i, to_sib, dp).wait_send()

        x_copy(p, zs, i, dp).wait_send()
        y_copy(p, zs, i, dp).wait_send()
        dy_copy(p, zs, i, dpx).wait_send()
        dx_copy(p, zs, i, dpy).wait_send()
        s_copy(p, zs, i).wait_send()

    def own_parts(p, act):
        @pl.when(p == 0)
        def _():
            act(wk_ref, 0, WIDE // 2, 0)
            act(wv_ref, 0, WIDE // 2, WIDE // 2)

        pl.when((p > 0) & (p < 5))(lambda: act(wq_ref, pl.multiple_of((p - 1) * WIDE, WIDE), WIDE, 0))
        pl.when(p >= 5)(lambda: act(wo_ref, pl.multiple_of((p - 5) * WIDE, WIDE), WIDE, 0))

    def send_own(p):
        mine = pl.ds(pl.multiple_of(dp * QUARTER, QUARTER), QUARTER)
        here = pl.ds(pl.multiple_of(c * T + dp * QUARTER, QUARTER), QUARTER)
        shard = pl.ds(pl.multiple_of(c * T, T), T)

        def act(ref, at, wide, to):
            src, dst = pl.ds(at, wide), pl.ds(to, wide)
            part, there = ref.at[mine, src], g_ref.at[p, z, here, dst]
            pl.when(z < 3)(lambda: remote(part, there, sup.at[p], rz.at[p, z], to_up).start())
            pl.when(z > 0)(lambda: remote(part, there, sdown.at[p], rz.at[p, z], to_down).start())
            remote(ref.at[:, src], g_ref.at[p, z, shard, dst], sown.at[p], rs.at[p, z], to_sib).start()

        own_parts(p, act)

    def own_sent(p, _):
        part = region(p, z, dp * QUARTER, QUARTER)
        pl.when(z < 3)(lambda: move(part, sup.at[p], rz.at[p, z], to_up).wait_send())
        pl.when(z > 0)(lambda: move(part, sdown.at[p], rz.at[p, z], to_down).wait_send())
        move(region(p, z, 0, T), sown.at[p], rs.at[p, z], to_sib).wait_send()

    def norm():
        x_load.wait()
        lane = lax.broadcasted_iota(jnp.int32, (T, HEAD), 1) < HEAD // 2
        table = turn_ref[...]
        other = pltpu.roll(table, HEAD // 2, 1)
        cos_s[...] = jnp.where(lane, table, other)
        sin_s[...] = jnp.where(lane, -other, table)

        def rows(i, _):
            at = pl.ds(pl.multiple_of(i * 16, 16), 16)
            wide = x_s[at, :].astype(F32)
            scale = lax.rsqrt(jnp.mean(wide * wide, -1, keepdims=True) + 1e-6)
            lhs_s[0, at, :] = (wide * scale * gain_ref[...].astype(F32)).astype(BF16)

        lax.fori_loop(0, T // 16, rows, None)

    def unit_source(m):
        return jnp.where(m == 0, z, source(m - 1))

    def load_unit(i):
        p, m, at = i // 4, i % 4, i % 2
        zs = unit_source(m)
        mine, other = pl.ds(pl.multiple_of(c * T, T), T), pl.ds(pl.multiple_of((1 - c) * T, T), T)
        there = g_ref.at[p, zs, other, :]
        remote(there, there, sown.at[0], rs.at[p, zs], to_sib).wait_recv()

        @pl.when(m == 0)
        def _():
            pltpu.make_async_copy(there, w_s.at[at, other, :], load_sem.at[at]).start()
            own_parts(p, lambda ref, start, wide, to: pltpu.make_async_copy(
                ref.at[:, pl.ds(start, wide)], w_s.at[at, mine, pl.ds(to, wide)], load_sem.at[at]).start())

        pl.when(m > 0)(lambda: pltpu.make_async_copy(g_ref.at[p, zs], w_s.at[at], load_sem.at[at]).start())

    def turned(t):
        t = t.astype(BF16).astype(F32)
        return (t * cos_s[...] + pltpu.roll(t, HEAD // 2, 1) * sin_s[...]).astype(BF16)

    def work_unit(i):
        p, m, at = i // 4, i % 4, i % 2
        zs = unit_source(m)
        which = jnp.where(p < 5, 0, 1)
        pltpu.make_async_copy(g_ref.at[p, zs], w_s.at[at], load_sem.at[at]).wait()

        @pl.when(m == 0)
        def _():
            acc_s[...] = jnp.zeros((T, WIDE), F32)

        deep = pl.ds(pl.multiple_of(zs * WIDE, WIDE), WIDE)

        for j in range(0, WIDE, 256):
            acc_s[:, j : j + 256] += jnp.dot(lhs_s[which, :, deep], w_s[at, :, j : j + 256], preferred_element_type=F32)

        @pl.when((m == 3) & (p == 0))
        def _():
            for h in range(4):
                kv_s[sp, h, 0] = turned(acc_s[:, h * HEAD : (h + 1) * HEAD])
                kv_s[sp, h, 1] = acc_s[:, 512 + h * HEAD : 512 + (h + 1) * HEAD].astype(BF16)

        @pl.when((m == 3) & (p > 0) & (p < 5))
        def _():
            def head(n, _):
                q_s[(p - 1) * 8 + n] = turned(acc_s[:, pl.ds(pl.multiple_of(n * HEAD, HEAD), HEAD)])

            lax.fori_loop(0, 8, head, None)

        @pl.when((m == 3) & (p >= 5))
        def _():
            def part(n, _):
                cols = pl.ds(pl.multiple_of((p - 5) * WIDE + n * 256, 256), 256)
                y_ref[:, cols] = (x_s[:, cols].astype(F32) + acc_s[:, pl.ds(pl.multiple_of(n * 256, 256), 256)]).astype(BF16)

            lax.fori_loop(0, WIDE // 256, part, None)

    def take(i):
        load_unit(i)
        pl.when(i > 0)(lambda: work_unit(i - 1))

    def kv_up(src, h, j):
        return move(kv_s.at[src, h], skv_up.at[j, h], rkv.at[src // 2, h], to_up)

    def kv_across(src, h, j):
        return move(kv_s.at[src, h], skv_sib.at[j, h], rskv.at[src // 2, h], to_sib)

    def kv_out(h):
        pl.when(z < 3)(lambda: kv_up(sp, h, 0).start())
        kv_across(sp, h, 0).start()

    def kv_in(i):
        chips = jnp.maximum(z, 1)
        h, j = i // chips, 1 + i % chips
        src = sp - 2 * j
        kv_up(src, h, j).wait_recv()
        pl.when(z < 3)(lambda: kv_up(src, h, j).start())
        kv_across(src, h, j).start()

    e = HEAD**-0.5 * LOG2E

    def block(h, src, masked):
        keys, values = kv_s[src, h, 0], kv_s[src, h, 1]
        scores = [_dot(keys, q_s[h * 8 + n], 1, 1) for n in range(8)]
        if masked:
            ok = lax.broadcasted_iota(jnp.int32, (T, T), 1) >= lax.broadcasted_iota(jnp.int32, (T, T), 0)
        weights, keeps = [], []
        for n, s in enumerate(scores):
            if masked:
                s = jnp.where(ok, s, HIDDEN)
            old = top_s[n : n + 1, :]
            top = jnp.maximum(old, s.max(axis=0, keepdims=True))
            top_s[n : n + 1, :] = top
            weights.append(jnp.exp2((s - top) * e).astype(BF16))
            keeps.append(jnp.exp2((old - top) * e))
        values = jnp.concatenate([values.T, jnp.ones((8, T), BF16)], axis=0)
        for n, (p, keep) in enumerate(zip(weights, keeps)):
            mix_s[n] = mix_s[n] * keep + _dot(values, p, 1, 0)

    def attend(i):
        blocks = 2 * z + 2
        h, j = i // blocks, i % blocks
        odd = j % 2
        src = 2 * (z - j // 2) + jnp.where(odd == 0, c, 1 - c)

        @pl.when(odd == 1)
        def _():
            kv_across(src, h, 0).wait_recv()

        @pl.when(j == 0)
        def _():
            top_s[...] = jnp.full((8, T), NEG, F32)
            mix_s[...] = jnp.zeros((8, HEAD + 8, T), F32)
            block(h, src, True)

        pl.when((j > 0) & (src < sp))(lambda: block(h, src, False))

        @pl.when(j == blocks - 1)
        def _():
            for n in range(8):
                at = pl.ds(pl.multiple_of(h * WIDE + n * HEAD, HEAD), HEAD)
                lhs_s[1, :, at] = (mix_s[n, :HEAD, :] * (1 / mix_s[n, HEAD : HEAD + 1, :])).T.astype(BF16)

    handlers = ((OWN, send_own), (Z_IN, z_in), (XY_OUT, xy_out), (XY_IN, xy_in), (D_IN, d_in), (TAKE, take), (KV_OUT, kv_out), (KV_IN, kv_in),
                (ATTEND, attend), (NORM, lambda i: norm()))

    def seven(g, counts):
        at, word = z * len(ORDERS[0]) + g, jnp.int32(0)
        for n, number in enumerate(sum(ORDERS, ())):
            word = jnp.where(at == n, number, word)

        def one(_, state):
            word, counts = state[0], state[1:]
            op = word % 16
            for (code, handler), count in zip(handlers, counts):
                pl.when(op == code)(functools.partial(handler, count))
            return (word // 16, *(count + jnp.where(op == code, 1, 0) for (code, _), count in zip(handlers, counts)))

        return lax.fori_loop(0, 7, one, (word, *counts))[1:]

    lax.fori_loop(0, len(ORDERS[0]), seven, (jnp.int32(0),) * len(handlers))
    work_unit(jnp.int32(4 * PHASES - 1))

    lax.fori_loop(0, PHASES, own_sent, None)
    lax.fori_loop(0, SLOTS, sent, None)

    def kv_sent(h, _):
        for j in range(4):
            @pl.when(z >= j)
            def _():
                pl.when(z < 3)(lambda: kv_up(sp - 2 * j, h, j).wait_send())
                kv_across(sp - 2 * j, h, j).wait_send()

    lax.fori_loop(0, 4, kv_sent, None)


def solution(mesh):
    dma = pltpu.SemaphoreType.DMA

    def step(x, gain, wq, wk, wv, wo):
        place = lax.axis_index("sp") * T + jnp.arange(T)
        half = HEAD // 2
        angle = place.astype(F32)[:, None] * THETA ** (-jnp.arange(half, dtype=F32) / half)
        turn = jnp.concatenate([jnp.cos(angle), jnp.sin(angle)], 1)
        hbm, vmem = pl.BlockSpec(memory_space=pltpu.HBM), pl.BlockSpec(memory_space=pltpu.VMEM)
        y, _ = pl.pallas_call(
            _kernel,
            in_specs=[hbm, vmem, hbm, hbm, hbm, hbm, vmem],
            out_specs=[vmem, hbm],
            out_shape=[pltpu.VMEM((T, D), BF16), jax.ShapeDtypeStruct((PHASES, 4, 2 * T, WIDE), BF16)],
            scratch_shapes=[
                pltpu.VMEM((T, D), BF16), pltpu.VMEM((2, T, D), BF16), pltpu.VMEM((32, T, HEAD), BF16), pltpu.VMEM((8, 4, 2, T, HEAD), BF16),
                pltpu.VMEM((T, WIDE), F32), pltpu.VMEM((2, 2 * T, WIDE), BF16), pltpu.VMEM((8, HEAD + 8, T), F32), pltpu.VMEM((8, T), F32),
                pltpu.VMEM((T, HEAD), F32), pltpu.VMEM((T, HEAD), F32),
                *[dma((PHASES, 4))] * 6, *[dma((SLOTS,))] * 6, *[dma((PHASES,))] * 3,
                dma((4, 4)), dma((4, 4)), dma((4, 4)), dma((4, 4)), dma((2,)), dma((1,)),
            ],
            compiler_params=pltpu.CompilerParams(collective_id=0, has_side_effects=True, vmem_limit_bytes=VMEM),
            cost_estimate=pl.CostEstimate(flops=2 * T * D * (2 * D + 1024) + 4 * T * D * D, transcendentals=32 * T * D, bytes_accessed=2**28),
        )(x, gain, wk, wv, wq, wo, turn)
        return y

    tokens, whole = P(("dp", "sp"), None), P("sp", None)
    return jax.shard_map(
        step,
        mesh=mesh,
        in_specs=(tokens, P(None), whole, whole, whole, whole),
        out_specs=tokens,
        check_vma=False,
    )
```

```python
import functools

import jax
import jax.numpy as jnp
from jax import lax
from jax.experimental import pallas as pl
from jax.experimental.pallas import tpu as pltpu
from jax.sharding import PartitionSpec as P

MESH = pl.DeviceIdType.MESH
NEG = -1e30
HIDDEN = 2 * NEG
LOG2E = 1.4426950408889634
VMEM = 56 * 2**20
HEAD = 128
THETA = 10000
T = 512
D = 4096
WIDE = 1024
PHASES = 9
SLOTS = 3 * PHASES
QUARTER = T // 4
BEHIND, LATE = 3, 5
F32 = jnp.float32
BF16 = jnp.bfloat16

OWN, Z_IN, XY_OUT, XY_IN, D_IN, TAKE, KV_OUT, KV_IN, ATTEND, NORM, WORK = range(1, 12)
DIRECT = 7
ORDERS = (
    (
        0x32b6a11, 0x4312432, 0x2254b65, 0x12b6533, 0x2534342, 0x1247b66, 0xbb63257, 0x625b346, 0x32124b6, 0x549695b,
        0x34b6b23, 0xb665212, 0x9725b34, 0x6b53496, 0x521234b, 0x5b34b66, 0x5b34969, 0x62534b6, 0x25b34b6, 0x534b621,
        0x66534b6, 0x3442534, 0x3722555, 0x4b29349, 0xb65b634, 0x655b6b6, 0x6b64b6b, 0x325bb6b, 0xb654b6, 0x0,
        0x0, 0x0, 0x0, 0x0,
    ),
    (
        0x32b6a11, 0x2343122, 0x4b65342, 0x4522123, 0x412b653, 0xb662532, 0xb635477, 0x346212b, 0x4b6685b, 0x26925b3,
        0xb348921, 0x5967295, 0x4b66b34, 0x49695b3, 0x22125b3, 0x3459689, 0xb34b66b, 0xb349695, 0x2124959, 0x662b563,
        0xb65b34b, 0x34b6534, 0x4534665, 0x9272253, 0x5533449, 0x4998345, 0xb6325b4, 0x6b655b6, 0x6b64b6b, 0x65b6b6b,
        0xb6bb, 0x0, 0x0, 0x0,
    ),
    (
        0x32b6a11, 0x2343122, 0x4b65342, 0x4522123, 0x412b653, 0xb662532, 0xb635477, 0x346212b, 0xb26685b, 0x9695b34,
        0x5889b34, 0x2126349, 0x7249b59, 0x6b86563, 0xb21234b, 0x3489695, 0x346959b, 0x286b596, 0xb34b212, 0xb349695,
        0x3496695, 0x349695b, 0xb634b95, 0x2223465, 0x5349957, 0x9853344, 0x3224955, 0x5985344, 0x6b6b495, 0x6b65b6b,
        0xb6b6b6b, 0x6b6b6b6, 0xbb, 0x0,
    ),
    (
        0x32b6a11, 0x4312432, 0x2254b65, 0x12b6533, 0x2534342, 0x1247b66, 0xbb63257, 0x625b346, 0x5b348b6, 0x5b34969,
        0x4962129, 0xb2665b3, 0x6958b34, 0x5b34889, 0x5b49689, 0x6693212, 0x72b5934, 0x59b34b6, 0x4588969, 0x432129b,
        0x96b5963, 0x9859324, 0x9958964, 0x9332124, 0x4b29595, 0x42b6b63, 0x2596372, 0x8b634b9, 0x3489956, 0x34b2959,
        0xb499586, 0xb6b6b65, 0x65b64b6, 0xb6b56bb,
    ),
)


def _dot(a, b, ca, cb):
    return lax.dot_general(a, b, (((ca,), (cb,)), ((), ())), preferred_element_type=F32)


def _kernel(x_ref, gain_ref, wk_ref, wv_ref, wq_ref, wo_ref, rate_ref, y_ref, g_ref,
            x_s, lhs_s, q_s, kv_s, acc_s, w_s, mix_s, top_s, cos_s, sin_s,
            rz, rx, ry, rdx, rdy, rs, sz, sx, sy, sdx, sdy, ss, sup, sdown, sown,
            rkv, rskv, skv_up, skv_sib, load_sem, x_sem):
    dp, sp = lax.axis_index("dp"), lax.axis_index("sp")
    xq, yq = dp // 2, dp % 2
    z, c = sp // 2, sp % 2
    dpx, dpy = (1 - xq) * 2 + yq, xq * 2 + (1 - yq)
    dpd = 3 - dp
    to_x, to_y, to_sib = (dpx, sp), (dpy, sp), (dp, z * 2 + (1 - c))
    to_up, to_down = (dp, sp + 2), (dp, sp - 2)

    x_load = pltpu.make_async_copy(x_ref, x_s, x_sem.at[0])
    x_load.start()
    barrier = pltpu.get_barrier_semaphore()
    for there in (to_x, to_y, to_sib):
        pl.semaphore_signal(barrier, inc=1, device_id=there, device_id_type=MESH)

    @pl.when(z < 3)
    def _():
        pl.semaphore_signal(barrier, inc=1, device_id=to_up, device_id_type=MESH)

    @pl.when(z > 0)
    def _():
        pl.semaphore_signal(barrier, inc=1, device_id=to_down, device_id_type=MESH)

    pl.semaphore_wait(barrier, 4 + ((z + 1) // 2) % 2)

    def source(k):
        a, b, d = (k - 1) * (k - 2) // 2, k * (2 - k), k * (k - 1) // 2
        return a * (1 + z % 2) + b * (2 - 2 * (z % 2) + z // 2) + d * (3 * (1 - z // 2))

    def region(p, zs, row, rows):
        return g_ref.at[p, zs, pl.ds(pl.multiple_of(c * T + row, 64), rows), :]

    def remote(src, dst, send, recv, there):
        return pltpu.make_async_remote_copy(src_ref=src, dst_ref=dst, send_sem=send, recv_sem=recv, device_id=there, device_id_type=MESH)

    def move(at, send, recv, there):
        return remote(at, at, send, recv, there)

    def z_copy(p, zs, i, there, quarter):
        return move(region(p, zs, quarter * QUARTER, QUARTER), sz.at[i], rz.at[p, zs], there)

    def x_copy(p, zs, i, quarter):
        return move(region(p, zs, quarter * QUARTER, QUARTER), sx.at[i], rx.at[p, zs], to_x)

    def y_copy(p, zs, i, quarter):
        return move(region(p, zs, quarter * QUARTER, QUARTER), sy.at[i], ry.at[p, zs], to_y)

    def dy_copy(p, zs, i, quarter):
        return move(region(p, zs, quarter * QUARTER, QUARTER // 2), sdy.at[i], rdy.at[p, zs], to_y)

    def dx_copy(p, zs, i, quarter):
        return move(region(p, zs, quarter * QUARTER + QUARTER // 2, QUARTER // 2), sdx.at[i], rdx.at[p, zs], to_x)

    def s_copy(p, zs, i):
        return move(region(p, zs, 0, T), ss.at[i], rs.at[p, zs], to_sib)

    def slot(i):
        i = jnp.where(i == 1, 3, jnp.where((i == 2) | (i == 3), i - 1, i))
        return i // 3, source(i % 3)

    def direct(p, zs):
        return (p >= DIRECT) & (((z == 0) & (zs == 1)) | ((z == 1) & (zs == 0)) | ((z == 2) & (zs == 3)))

    def z_in(i):
        p, zs = slot(i)
        whole = direct(p, zs)
        pl.when(jnp.logical_not(whole))(lambda: z_copy(p, zs, i, to_sib, dp).wait_recv())

        @pl.when(whole)
        def _():
            move(region(p, zs, 0, T), sz.at[i], rz.at[p, zs], to_sib).wait_recv()
            s_copy(p, zs, i).start()

        @pl.when((zs < z) & (z < 3))
        def _():
            z_copy(p, zs, i, to_up, dp).start()

        @pl.when((zs > z) & (z > 0))
        def _():
            z_copy(p, zs, i, to_down, dp).start()

    def unless_direct(act):
        def handler(i):
            p, zs = slot(i)
            pl.when(jnp.logical_not(direct(p, zs)))(lambda: act(p, zs, i))

        return handler

    def xy_out(p, zs, i):
        x_copy(p, zs, i, dp).start()
        y_copy(p, zs, i, dp).start()

    def xy_in(p, zs, i):
        x_copy(p, zs, i, dpx).wait_recv()
        dy_copy(p, zs, i, dpx).start()
        y_copy(p, zs, i, dpy).wait_recv()
        dx_copy(p, zs, i, dpy).start()

    def d_in(p, zs, i):
        dy_copy(p, zs, i, dpd).wait_recv()
        dx_copy(p, zs, i, dpd).wait_recv()
        s_copy(p, zs, i).start()

    def d_in_and_sent(i):
        unless_direct(d_in)(i)
        pl.when(i >= LATE)(lambda: sent(i - LATE, None))

    def sent(i, _):
        p, zs = slot(i)

        @pl.when(((zs < z) & (z < 3)) | ((zs > z) & (z > 0)))
        def _():
            z_copy(p, zs, i, to_sib, dp).wait_send()

        @pl.when(jnp.logical_not(direct(p, zs)))
        def _():
            x_copy(p, zs, i, dp).wait_send()
            y_copy(p, zs, i, dp).wait_send()
            dy_copy(p, zs, i, dpx).wait_send()
            dx_copy(p, zs, i, dpy).wait_send()

        s_copy(p, zs, i).wait_send()

    def own_parts(p, act):
        @pl.when(p == 0)
        def _():
            act(wk_ref, 0, WIDE // 2, 0)
            act(wv_ref, 0, WIDE // 2, WIDE // 2)

        pl.when((p > 0) & (p < 5))(lambda: act(wq_ref, pl.multiple_of((p - 1) * WIDE, WIDE), WIDE, 0))
        pl.when(p >= 5)(lambda: act(wo_ref, pl.multiple_of((p - 5) * WIDE, WIDE), WIDE, 0))

    def whole_up(p):
        return (p >= DIRECT) & (z == 0)

    def whole_down(p):
        return (p >= DIRECT) & ((z == 1) | (z == 3))

    def send_own(p):
        mine = pl.ds(pl.multiple_of(dp * QUARTER, QUARTER), QUARTER)
        here = pl.ds(pl.multiple_of(c * T + dp * QUARTER, QUARTER), QUARTER)
        shard = pl.ds(pl.multiple_of(c * T, T), T)

        def act(ref, at, wide, to):
            src, dst = pl.ds(at, wide), pl.ds(to, wide)
            part, there = ref.at[mine, src], g_ref.at[p, z, here, dst]
            all_rows, all_there = ref.at[:, src], g_ref.at[p, z, shard, dst]
            pl.when((z < 3) & jnp.logical_not(whole_up(p)))(lambda: remote(part, there, sup.at[p], rz.at[p, z], to_up).start())
            pl.when(whole_up(p))(lambda: remote(all_rows, all_there, sup.at[p], rz.at[p, z], to_up).start())
            pl.when((z > 0) & jnp.logical_not(whole_down(p)))(lambda: remote(part, there, sdown.at[p], rz.at[p, z], to_down).start())
            pl.when(whole_down(p))(lambda: remote(all_rows, all_there, sdown.at[p], rz.at[p, z], to_down).start())
            remote(all_rows, all_there, sown.at[p], rs.at[p, z], to_sib).start()

        own_parts(p, act)
        pl.when(p >= BEHIND)(lambda: own_sent(p - BEHIND, None))

    def own_sent(p, _):
        part, rows = region(p, z, dp * QUARTER, QUARTER), region(p, z, 0, T)
        pl.when((z < 3) & jnp.logical_not(whole_up(p)))(lambda: move(part, sup.at[p], rz.at[p, z], to_up).wait_send())
        pl.when(whole_up(p))(lambda: move(rows, sup.at[p], rz.at[p, z], to_up).wait_send())
        pl.when((z > 0) & jnp.logical_not(whole_down(p)))(lambda: move(part, sdown.at[p], rz.at[p, z], to_down).wait_send())
        pl.when(whole_down(p))(lambda: move(rows, sdown.at[p], rz.at[p, z], to_down).wait_send())
        move(rows, sown.at[p], rs.at[p, z], to_sib).wait_send()

    def norm():
        x_load.wait()
        def rows(i, _):
            at = pl.ds(pl.multiple_of(i * 16, 16), 16)
            wide = x_s[at, :].astype(F32)
            scale = lax.rsqrt(jnp.mean(wide * wide, -1, keepdims=True) + 1e-6)
            lhs_s[0, at, :] = (wide * scale * gain_ref[...].astype(F32)).astype(BF16)

        lax.fori_loop(0, T // 16, rows, None)

    def unit(i):
        j, special = i - 20, (z == 3) & (i >= 20) & (i < 28)
        early = j < 6
        p = jnp.where(special, jnp.where(early, 5 + j // 3, j - 1), i // 4)
        m = jnp.where(special, jnp.where(early, 1 + j % 3, 0), i % 4)
        return p, m, m == jnp.where(special, 0, 3)

    def unit_source(m):
        return jnp.where(m == 0, z, source(m - 1))

    def load_unit(i):
        (p, m, _), at = unit(i), i % 2
        zs = unit_source(m)
        mine, other = pl.ds(pl.multiple_of(c * T, T), T), pl.ds(pl.multiple_of((1 - c) * T, T), T)
        there = g_ref.at[p, zs, other, :]
        remote(there, there, sown.at[0], rs.at[p, zs], to_sib).wait_recv()

        @pl.when(m == 0)
        def _():
            pltpu.make_async_copy(there, w_s.at[at, other, :], load_sem.at[at]).start()
            own_parts(p, lambda ref, start, wide, to: pltpu.make_async_copy(
                ref.at[:, pl.ds(start, wide)], w_s.at[at, mine, pl.ds(to, wide)], load_sem.at[at]).start())

        pl.when(m > 0)(lambda: pltpu.make_async_copy(g_ref.at[p, zs], w_s.at[at], load_sem.at[at]).start())

    def turned(t):
        t = t.astype(BF16).astype(F32)
        return (t * cos_s[...] + pltpu.roll(t, HEAD // 2, 1) * sin_s[...]).astype(BF16)

    def work_unit(i):
        (p, m, last), at = unit(i), i % 2
        zs = unit_source(m)
        which, base = jnp.where(p < 5, 0, 1), jnp.where(p < 5, 0, p - 5) * WIDE
        pltpu.make_async_copy(g_ref.at[p, zs], w_s.at[at], load_sem.at[at]).wait()

        @pl.when(i == 0)
        def _():
            place = (sp * T + lax.broadcasted_iota(jnp.int32, (T, HEAD), 0)).astype(F32)
            angle = place * rate_ref[...]
            cos_s[...] = jnp.cos(angle)
            sine = jnp.sin(angle)
            sin_s[...] = jnp.where(lax.broadcasted_iota(jnp.int32, (T, HEAD), 1) < HEAD // 2, -sine, sine)

        @pl.when((m == 0) & (p < 5))
        def _():
            acc_s[:, :WIDE] = jnp.zeros((T, WIDE), F32)

        @pl.when(i == 20)
        def _():
            acc_s[...] = jnp.zeros((T, D), F32)

        deep = pl.ds(pl.multiple_of(zs * WIDE, WIDE), WIDE)
        for j in range(0, WIDE, 256):
            cols = pl.ds(pl.multiple_of(base + j, 256), 256)
            acc_s[:, cols] += jnp.dot(lhs_s[which, :, deep], w_s[at, :, j : j + 256], preferred_element_type=F32)

        @pl.when(last & (p == 0))
        def _():
            for h in range(4):
                kv_s[sp, h, 0] = turned(acc_s[:, h * HEAD : (h + 1) * HEAD])
                kv_s[sp, h, 1] = acc_s[:, 512 + h * HEAD : 512 + (h + 1) * HEAD].astype(BF16)

        @pl.when(last & (p > 0) & (p < 5))
        def _():
            def head(n, _):
                q_s[(p - 1) * 8 + n] = turned(acc_s[:, pl.ds(pl.multiple_of(n * HEAD, HEAD), HEAD)])

            lax.fori_loop(0, 8, head, None)

        @pl.when(last & (p >= 5))
        def _():
            def part(n, _):
                cols = pl.ds(pl.multiple_of((p - 5) * WIDE + n * 256, 256), 256)
                y_ref[:, cols] = (x_s[:, cols].astype(F32) + acc_s[:, cols]).astype(BF16)

            lax.fori_loop(0, WIDE // 256, part, None)

    def kv_up(src, h, j):
        return move(kv_s.at[src, h], skv_up.at[j, h], rkv.at[src // 2, h], to_up)

    def kv_across(src, h, j):
        return move(kv_s.at[src, h], skv_sib.at[j, h], rskv.at[src // 2, h], to_sib)

    def kv_out(h):
        pl.when(z < 3)(lambda: kv_up(sp, h, 0).start())
        kv_across(sp, h, 0).start()

    def kv_in(i):
        chips = jnp.maximum(z, 1)
        h, j = i // chips, 1 + i % chips
        src = sp - 2 * j
        kv_up(src, h, j).wait_recv()
        pl.when(z < 3)(lambda: kv_up(src, h, j).start())
        kv_across(src, h, j).start()

    e = HEAD**-0.5 * LOG2E

    def block(h, src, masked):
        keys, values = kv_s[src, h, 0], kv_s[src, h, 1]
        scores = [_dot(keys, q_s[h * 8 + n], 1, 1) for n in range(8)]
        if masked:
            ok = lax.broadcasted_iota(jnp.int32, (T, T), 1) >= lax.broadcasted_iota(jnp.int32, (T, T), 0)
        weights, keeps = [], []
        for n, s in enumerate(scores):
            if masked:
                s = jnp.where(ok, s, HIDDEN)
            old = top_s[n : n + 1, :]
            top = jnp.maximum(old, s.max(axis=0, keepdims=True))
            top_s[n : n + 1, :] = top
            weights.append(jnp.exp2((s - top) * e).astype(BF16))
            keeps.append(jnp.exp2((old - top) * e))
        values = jnp.concatenate([values.T, jnp.ones((8, T), BF16)], axis=0)
        for n, (p, keep) in enumerate(zip(weights, keeps)):
            mix_s[n] = mix_s[n] * keep + _dot(values, p, 1, 0)

    def attend(i):
        blocks = 2 * z + 2
        h, j = i // blocks, i % blocks
        odd = j % 2
        src = 2 * (z - j // 2) + jnp.where(odd == 0, c, 1 - c)

        @pl.when(odd == 1)
        def _():
            kv_across(src, h, 0).wait_recv()

        @pl.when(j == 0)
        def _():
            top_s[...] = jnp.full((8, T), NEG, F32)
            mix_s[...] = jnp.zeros((8, HEAD + 8, T), F32)
            block(h, src, True)

        pl.when((j > 0) & (src < sp))(lambda: block(h, src, False))

        @pl.when(j == blocks - 1)
        def _():
            for n in range(8):
                at = pl.ds(pl.multiple_of(h * WIDE + n * HEAD, HEAD), HEAD)
                lhs_s[1, :, at] = (mix_s[n, :HEAD, :] * (1 / mix_s[n, HEAD : HEAD + 1, :])).T.astype(BF16)

    handlers = ((OWN, send_own), (Z_IN, z_in), (XY_OUT, unless_direct(xy_out)), (XY_IN, unless_direct(xy_in)), (D_IN, d_in_and_sent),
                (TAKE, load_unit), (KV_OUT, kv_out), (KV_IN, kv_in), (ATTEND, attend), (NORM, lambda i: norm()), (WORK, work_unit))

    def seven(g, counts):
        at, word = z * len(ORDERS[0]) + g, jnp.int32(0)
        for n, number in enumerate(sum(ORDERS, ())):
            word = jnp.where(at == n, number, word)

        def one(_, state):
            word, counts = state[0], state[1:]
            op = word % 16
            for (code, handler), count in zip(handlers, counts):
                pl.when(op == code)(functools.partial(handler, count))
            return (word // 16, *(count + jnp.where(op == code, 1, 0) for (code, _), count in zip(handlers, counts)))

        return lax.fori_loop(0, 7, one, (word, *counts))[1:]

    lax.fori_loop(0, len(ORDERS[0]), seven, (jnp.int32(0),) * len(handlers))

    lax.fori_loop(PHASES - BEHIND, PHASES, own_sent, None)
    lax.fori_loop(SLOTS - LATE, SLOTS, sent, None)

    def kv_sent(h, _):
        for j in range(4):
            @pl.when(z >= j)
            def _():
                pl.when(z < 3)(lambda: kv_up(sp - 2 * j, h, j).wait_send())
                kv_across(sp - 2 * j, h, j).wait_send()

    lax.fori_loop(0, 4, kv_sent, None)


def solution(mesh):
    dma = pltpu.SemaphoreType.DMA

    def step(x, gain, wq, wk, wv, wo):
        rate = THETA ** (-jnp.arange(HEAD // 2, dtype=F32) / (HEAD // 2))
        rate = jnp.concatenate([rate, rate])[None]
        hbm, vmem = pl.BlockSpec(memory_space=pltpu.HBM), pl.BlockSpec(memory_space=pltpu.VMEM)
        y, _ = pl.pallas_call(
            _kernel,
            in_specs=[hbm, vmem, hbm, hbm, hbm, hbm, vmem],
            out_specs=[vmem, hbm],
            out_shape=[pltpu.VMEM((T, D), BF16), jax.ShapeDtypeStruct((PHASES, 4, 2 * T, WIDE), BF16)],
            scratch_shapes=[
                pltpu.VMEM((T, D), BF16), pltpu.VMEM((2, T, D), BF16), pltpu.VMEM((32, T, HEAD), BF16), pltpu.VMEM((8, 4, 2, T, HEAD), BF16),
                pltpu.VMEM((T, D), F32), pltpu.VMEM((2, 2 * T, WIDE), BF16), pltpu.VMEM((8, HEAD + 8, T), F32), pltpu.VMEM((8, T), F32),
                pltpu.VMEM((T, HEAD), F32), pltpu.VMEM((T, HEAD), F32),
                *[dma((PHASES, 4))] * 6, *[dma((SLOTS,))] * 6, *[dma((PHASES,))] * 3,
                dma((4, 4)), dma((4, 4)), dma((4, 4)), dma((4, 4)), dma((2,)), dma((1,)),
            ],
            compiler_params=pltpu.CompilerParams(collective_id=0, has_side_effects=True, vmem_limit_bytes=VMEM),
            cost_estimate=pl.CostEstimate(flops=2 * T * D * (2 * D + 1024) + 4 * T * D * D, transcendentals=32 * T * D, bytes_accessed=2**28),
        )(x, gain, wk, wv, wq, wo, rate)
        return y

    tokens, whole = P(("dp", "sp"), None), P("sp", None)
    return jax.shard_map(
        step,
        mesh=mesh,
        in_specs=(tokens, P(None), whole, whole, whole, whole),
        out_specs=tokens,
        check_vma=False,
    )
```

```python
import functools

import jax
import jax.numpy as jnp
from jax import lax
from jax.experimental import pallas as pl
from jax.experimental.pallas import tpu as pltpu
from jax.sharding import PartitionSpec as P

MESH = pl.DeviceIdType.MESH
NEG = -1e30
HIDDEN = 2 * NEG
LOG2E = 1.4426950408889634
VMEM = 56 * 2**20
HEAD = 128
THETA = 10000
T = 512
D = 4096
WIDE = 1024
PHASES = 9
SLOTS = 3 * PHASES
QUARTER = T // 4
BEHIND, LATE = 3, 5
F32 = jnp.float32
BF16 = jnp.bfloat16

OWN, Z_IN, XY_OUT, XY_IN, D_IN, TAKE, KV_OUT, KV_IN, ATTEND, NORM, WORK = range(1, 12)
DIRECT = 7
ORDERS = (
    (
        0x32b6a11, 0x4312432, 0x2254b65, 0x12b6533, 0x2534342, 0x1247b66, 0xbb63257, 0x625b346, 0x32124b6, 0x549695b,
        0x34b6b23, 0xb665212, 0x9725b34, 0x6b53496, 0x521234b, 0x5b34b66, 0x5b34969, 0x62534b6, 0x32124b6, 0x534b65b,
        0x66534b6, 0x3442534, 0x3272555, 0x4b29349, 0xb65b634, 0x655b6b6, 0x6b64b6b, 0x325bb6b, 0xb654b6, 0x0,
        0x0, 0x0, 0x0, 0x0,
    ),
    (
        0x32b6a11, 0x2343122, 0x4b65342, 0x4225123, 0x234b653, 0xb662521, 0xb635477, 0x4b2126b, 0x4b86653, 0x96925b3,
        0xb321248, 0x5967295, 0x4b66b34, 0x49695b3, 0x22125b3, 0x3458969, 0xb34b66b, 0xb349695, 0x2634959, 0x662b521,
        0xb65b34b, 0x34b6534, 0x4534665, 0x9227253, 0x5533449, 0x4998345, 0xb6325b4, 0x6b655b6, 0x6b6b64b, 0x6b65b6b,
        0xbb6b, 0x0, 0x0, 0x0,
    ),
    (
        0x32b6a11, 0x2343122, 0x4b65342, 0x4225123, 0x234b653, 0xb662521, 0xb635477, 0x4b2126b, 0xb266853, 0x9695b34,
        0x5889b34, 0x2596349, 0x2489b21, 0x6b66537, 0x125b34b, 0x3489692, 0x496695b, 0x489b5b3, 0x9632122, 0x56349b5,
        0x34b6b69, 0x9349695, 0xb634b95, 0x2523465, 0x5349927, 0x9853344, 0x3224955, 0x5985344, 0x6b6b495, 0x6b65b6b,
        0xb6b6b6b, 0x6b6b6b6, 0xbb, 0x0,
    ),
    (
        0x32b6a11, 0x4312432, 0x2254b65, 0x12b6533, 0x2534342, 0x1247b66, 0xbb63257, 0x625b346, 0x5b348b6, 0x5b34969,
        0x4962129, 0xb2665b3, 0x6958b34, 0x5b34889, 0x5b49689, 0x6693212, 0x72b5934, 0x89b34b6, 0x4589695, 0x432129b,
        0x96b5963, 0x9859324, 0x9958964, 0x9332124, 0x4b29595, 0x72b6b63, 0x5896324, 0x5932499, 0x934986b, 0x34b6b25,
        0xb495986, 0x64b6b56, 0x65b6b6b, 0xbb66b5b,
    ),
)


def _dot(a, b, ca, cb):
    return lax.dot_general(a, b, (((ca,), (cb,)), ((), ())), preferred_element_type=F32)


def _kernel(x_ref, gain_ref, wk_ref, wv_ref, wq_ref, wo_ref, rate_ref, y_ref, g_ref,
            x_s, lhs_s, q_s, kv_s, acc_s, w_s, mix_s, top_s, cos_s, sin_s,
            rz, rx, ry, rdx, rdy, rs, sz, sx, sy, sdx, sdy, ss, sup, sdown, sown,
            rlast, rkv, rskv, skv_up, skv_sib, load_sem, x_sem):
    dp, sp = lax.axis_index("dp"), lax.axis_index("sp")
    xq, yq = dp // 2, dp % 2
    z, c = sp // 2, sp % 2
    dpx, dpy = (1 - xq) * 2 + yq, xq * 2 + (1 - yq)
    dpd = 3 - dp
    to_x, to_y, to_sib = (dpx, sp), (dpy, sp), (dp, z * 2 + (1 - c))
    to_up, to_down = (dp, sp + 2), (dp, sp - 2)

    x_load = pltpu.make_async_copy(x_ref, x_s, x_sem.at[0])
    x_load.start()
    barrier = pltpu.get_barrier_semaphore()
    for there in (to_x, to_y, to_sib):
        pl.semaphore_signal(barrier, inc=1, device_id=there, device_id_type=MESH)

    @pl.when(z < 3)
    def _():
        pl.semaphore_signal(barrier, inc=1, device_id=to_up, device_id_type=MESH)

    @pl.when(z > 0)
    def _():
        pl.semaphore_signal(barrier, inc=1, device_id=to_down, device_id_type=MESH)

    pl.semaphore_wait(barrier, 4 + ((z + 1) // 2) % 2)

    def source(k):
        a, b, d = (k - 1) * (k - 2) // 2, k * (2 - k), k * (k - 1) // 2
        return a * (1 + z % 2) + b * (2 - 2 * (z % 2) + z // 2) + d * (3 * (1 - z // 2))

    def region(p, zs, row, rows):
        return g_ref.at[p, zs, pl.ds(pl.multiple_of(c * T + row, 64), rows), :]

    def remote(src, dst, send, recv, there):
        return pltpu.make_async_remote_copy(src_ref=src, dst_ref=dst, send_sem=send, recv_sem=recv, device_id=there, device_id_type=MESH)

    def move(at, send, recv, there):
        return remote(at, at, send, recv, there)

    def z_copy(p, zs, i, there, quarter):
        return move(region(p, zs, quarter * QUARTER, QUARTER), sz.at[i], rz.at[p, zs], there)

    def x_copy(p, zs, i, quarter):
        return move(region(p, zs, quarter * QUARTER, QUARTER), sx.at[i], rx.at[p, zs], to_x)

    def y_copy(p, zs, i, quarter):
        return move(region(p, zs, quarter * QUARTER, QUARTER), sy.at[i], ry.at[p, zs], to_y)

    def dy_copy(p, zs, i, quarter):
        return move(region(p, zs, quarter * QUARTER, QUARTER // 2), sdy.at[i], rdy.at[p, zs], to_y)

    def dx_copy(p, zs, i, quarter):
        return move(region(p, zs, quarter * QUARTER + QUARTER // 2, QUARTER // 2), sdx.at[i], rdx.at[p, zs], to_x)

    def s_copy(p, zs, i):
        return move(region(p, zs, 0, T), ss.at[i], rs.at[p, zs], to_sib)

    def slot(i):
        i = jnp.where(i == 1, 3, jnp.where((i == 2) | (i == 3), i - 1, i))
        return i // 3, source(i % 3)

    def direct(p, zs):
        return (p >= DIRECT) & (((z == 0) & (zs == 1)) | ((z == 1) & (zs == 0)) | ((z == 2) & (zs == 3)))

    def z_in(i):
        p, zs = slot(i)
        whole = direct(p, zs)
        pl.when(jnp.logical_not(whole))(lambda: z_copy(p, zs, i, to_sib, dp).wait_recv())

        @pl.when(whole)
        def _():
            move(region(p, zs, 0, T), sz.at[i], rz.at[p, zs], to_sib).wait_recv()
            s_copy(p, zs, i).start()

        @pl.when((zs < z) & (z < 3))
        def _():
            z_copy(p, zs, i, to_up, dp).start()

        @pl.when((zs > z) & (z > 0))
        def _():
            z_copy(p, zs, i, to_down, dp).start()

    def unless_direct(act):
        def handler(i):
            p, zs = slot(i)
            pl.when(jnp.logical_not(direct(p, zs)))(lambda: act(p, zs, i))

        return handler

    def half(p, zs, quarter, n, send, recv, there):
        return move(region(p, zs, quarter * QUARTER + n * (QUARTER // 2), QUARTER // 2), send, recv, there)

    def xy_out(p, zs, i):
        @pl.when(i < SLOTS - 1)
        def _():
            x_copy(p, zs, i, dp).start()
            y_copy(p, zs, i, dp).start()

        @pl.when(i == SLOTS - 1)
        def _():
            half(p, zs, dp, 0, sx.at[i], rx.at[p, zs], to_x).start()
            half(p, zs, dp, 1, sy.at[i], ry.at[p, zs], to_y).start()
            half(p, zs, dp, 1, sx.at[i], rlast.at[0], to_x).start()
            half(p, zs, dp, 0, sy.at[i], rlast.at[1], to_y).start()

    def xy_in(p, zs, i):
        @pl.when(i < SLOTS - 1)
        def _():
            x_copy(p, zs, i, dpx).wait_recv()
            dy_copy(p, zs, i, dpx).start()
            y_copy(p, zs, i, dpy).wait_recv()
            dx_copy(p, zs, i, dpy).start()

        @pl.when(i == SLOTS - 1)
        def _():
            half(p, zs, dpx, 0, sx.at[i], rx.at[p, zs], to_x).wait_recv()
            dy_copy(p, zs, i, dpx).start()
            half(p, zs, dpy, 1, sy.at[i], ry.at[p, zs], to_y).wait_recv()
            dx_copy(p, zs, i, dpy).start()

    def d_in(p, zs, i):
        @pl.when(i == SLOTS - 1)
        def _():
            half(p, zs, dpx, 1, sx.at[i], rlast.at[0], to_x).wait_recv()
            half(p, zs, dpy, 0, sy.at[i], rlast.at[1], to_y).wait_recv()

        dy_copy(p, zs, i, dpd).wait_recv()
        dx_copy(p, zs, i, dpd).wait_recv()
        s_copy(p, zs, i).start()

    def d_in_and_sent(i):
        unless_direct(d_in)(i)
        pl.when(i >= LATE)(lambda: sent(i - LATE, None))

    def sent(i, _):
        p, zs = slot(i)

        @pl.when(((zs < z) & (z < 3)) | ((zs > z) & (z > 0)))
        def _():
            z_copy(p, zs, i, to_sib, dp).wait_send()

        @pl.when(jnp.logical_not(direct(p, zs)))
        def _():
            x_copy(p, zs, i, dp).wait_send()
            y_copy(p, zs, i, dp).wait_send()
            dy_copy(p, zs, i, dpx).wait_send()
            dx_copy(p, zs, i, dpy).wait_send()

        s_copy(p, zs, i).wait_send()

    def own_parts(p, act):
        @pl.when(p == 0)
        def _():
            act(wk_ref, 0, WIDE // 2, 0)
            act(wv_ref, 0, WIDE // 2, WIDE // 2)

        pl.when((p > 0) & (p < 5))(lambda: act(wq_ref, pl.multiple_of((p - 1) * WIDE, WIDE), WIDE, 0))
        pl.when(p >= 5)(lambda: act(wo_ref, pl.multiple_of((p - 5) * WIDE, WIDE), WIDE, 0))

    def whole_up(p):
        return (p >= DIRECT) & (z == 0)

    def whole_down(p):
        return (p >= DIRECT) & ((z == 1) | (z == 3))

    def send_own(p):
        mine = pl.ds(pl.multiple_of(dp * QUARTER, QUARTER), QUARTER)
        here = pl.ds(pl.multiple_of(c * T + dp * QUARTER, QUARTER), QUARTER)
        shard = pl.ds(pl.multiple_of(c * T, T), T)

        def act(ref, at, wide, to):
            src, dst = pl.ds(at, wide), pl.ds(to, wide)
            part, there = ref.at[mine, src], g_ref.at[p, z, here, dst]
            all_rows, all_there = ref.at[:, src], g_ref.at[p, z, shard, dst]
            pl.when((z < 3) & jnp.logical_not(whole_up(p)))(lambda: remote(part, there, sup.at[p], rz.at[p, z], to_up).start())
            pl.when(whole_up(p))(lambda: remote(all_rows, all_there, sup.at[p], rz.at[p, z], to_up).start())
            pl.when((z > 0) & jnp.logical_not(whole_down(p)))(lambda: remote(part, there, sdown.at[p], rz.at[p, z], to_down).start())
            pl.when(whole_down(p))(lambda: remote(all_rows, all_there, sdown.at[p], rz.at[p, z], to_down).start())
            remote(all_rows, all_there, sown.at[p], rs.at[p, z], to_sib).start()

        own_parts(p, act)
        pl.when(p >= BEHIND)(lambda: own_sent(p - BEHIND, None))

    def own_sent(p, _):
        part, rows = region(p, z, dp * QUARTER, QUARTER), region(p, z, 0, T)
        pl.when((z < 3) & jnp.logical_not(whole_up(p)))(lambda: move(part, sup.at[p], rz.at[p, z], to_up).wait_send())
        pl.when(whole_up(p))(lambda: move(rows, sup.at[p], rz.at[p, z], to_up).wait_send())
        pl.when((z > 0) & jnp.logical_not(whole_down(p)))(lambda: move(part, sdown.at[p], rz.at[p, z], to_down).wait_send())
        pl.when(whole_down(p))(lambda: move(rows, sdown.at[p], rz.at[p, z], to_down).wait_send())
        move(rows, sown.at[p], rs.at[p, z], to_sib).wait_send()

    def norm():
        x_load.wait()
        def rows(i, _):
            at = pl.ds(pl.multiple_of(i * 16, 16), 16)
            wide = x_s[at, :].astype(F32)
            scale = lax.rsqrt(jnp.mean(wide * wide, -1, keepdims=True) + 1e-6)
            lhs_s[0, at, :] = (wide * scale * gain_ref[...].astype(F32)).astype(BF16)

        lax.fori_loop(0, T // 16, rows, None)

    def unit(i):
        j, special = i - 20, (z == 3) & (i >= 20) & (i < 28)
        early = j < 6
        p = jnp.where(special, jnp.where(early, 5 + j // 3, j - 1), i // 4)
        m = jnp.where(special, jnp.where(early, 1 + j % 3, 0), i % 4)
        return p, m, m == jnp.where(special, 0, 3)

    def unit_source(m):
        return jnp.where(m == 0, z, source(m - 1))

    def load_unit(i):
        (p, m, _), at = unit(i), i % 2
        zs = unit_source(m)
        mine, other = pl.ds(pl.multiple_of(c * T, T), T), pl.ds(pl.multiple_of((1 - c) * T, T), T)
        there = g_ref.at[p, zs, other, :]
        remote(there, there, sown.at[0], rs.at[p, zs], to_sib).wait_recv()

        @pl.when(m == 0)
        def _():
            pltpu.make_async_copy(there, w_s.at[at, other, :], load_sem.at[at]).start()
            own_parts(p, lambda ref, start, wide, to: pltpu.make_async_copy(
                ref.at[:, pl.ds(start, wide)], w_s.at[at, mine, pl.ds(to, wide)], load_sem.at[at]).start())

        pl.when(m > 0)(lambda: pltpu.make_async_copy(g_ref.at[p, zs], w_s.at[at], load_sem.at[at]).start())

    def turned(t):
        t = t.astype(BF16).astype(F32)
        return (t * cos_s[...] + pltpu.roll(t, HEAD // 2, 1) * sin_s[...]).astype(BF16)

    def work_unit(i):
        (p, m, last), at = unit(i), i % 2
        zs = unit_source(m)
        which, base = jnp.where(p < 5, 0, 1), jnp.where(p < 5, 0, p - 5) * WIDE
        pltpu.make_async_copy(g_ref.at[p, zs], w_s.at[at], load_sem.at[at]).wait()

        @pl.when(i == 0)
        def _():
            place = (sp * T + lax.broadcasted_iota(jnp.int32, (T, HEAD), 0)).astype(F32)
            angle = place * rate_ref[...]
            cos_s[...] = jnp.cos(angle)
            sine = jnp.sin(angle)
            sin_s[...] = jnp.where(lax.broadcasted_iota(jnp.int32, (T, HEAD), 1) < HEAD // 2, -sine, sine)

        @pl.when((m == 0) & (p < 5))
        def _():
            acc_s[:, :WIDE] = jnp.zeros((T, WIDE), F32)

        @pl.when(i == 20)
        def _():
            acc_s[...] = jnp.zeros((T, D), F32)

        deep = pl.ds(pl.multiple_of(zs * WIDE, WIDE), WIDE)
        for j in range(0, WIDE, 256):
            cols = pl.ds(pl.multiple_of(base + j, 256), 256)
            acc_s[:, cols] += jnp.dot(lhs_s[which, :, deep], w_s[at, :, j : j + 256], preferred_element_type=F32)

        @pl.when(last & (p == 0))
        def _():
            for h in range(4):
                kv_s[sp, h, 0] = turned(acc_s[:, h * HEAD : (h + 1) * HEAD])
                kv_s[sp, h, 1] = acc_s[:, 512 + h * HEAD : 512 + (h + 1) * HEAD].astype(BF16)

        @pl.when(last & (p > 0) & (p < 5))
        def _():
            def head(n, _):
                q_s[(p - 1) * 8 + n] = turned(acc_s[:, pl.ds(pl.multiple_of(n * HEAD, HEAD), HEAD)])

            lax.fori_loop(0, 8, head, None)

        @pl.when(last & (p >= 5))
        def _():
            def part(n, _):
                cols = pl.ds(pl.multiple_of((p - 5) * WIDE + n * 256, 256), 256)
                y_ref[:, cols] = (x_s[:, cols].astype(F32) + acc_s[:, cols]).astype(BF16)

            lax.fori_loop(0, WIDE // 256, part, None)

    def kv_up(src, h, j):
        return move(kv_s.at[src, h], skv_up.at[j, h], rkv.at[src // 2, h], to_up)

    def kv_across(src, h, j):
        return move(kv_s.at[src, h], skv_sib.at[j, h], rskv.at[src // 2, h], to_sib)

    def kv_out(h):
        pl.when(z < 3)(lambda: kv_up(sp, h, 0).start())
        kv_across(sp, h, 0).start()

    def kv_in(i):
        chips = jnp.maximum(z, 1)
        h, j = i // chips, 1 + i % chips
        src = sp - 2 * j
        kv_up(src, h, j).wait_recv()
        pl.when(z < 3)(lambda: kv_up(src, h, j).start())
        kv_across(src, h, j).start()

    e = HEAD**-0.5 * LOG2E

    def block(h, src, masked):
        keys, values = kv_s[src, h, 0], kv_s[src, h, 1]
        scores = [_dot(keys, q_s[h * 8 + n], 1, 1) for n in range(8)]
        if masked:
            ok = lax.broadcasted_iota(jnp.int32, (T, T), 1) >= lax.broadcasted_iota(jnp.int32, (T, T), 0)
        weights, keeps = [], []
        for n, s in enumerate(scores):
            if masked:
                s = jnp.where(ok, s, HIDDEN)
            old = top_s[n : n + 1, :]
            top = jnp.maximum(old, s.max(axis=0, keepdims=True))
            top_s[n : n + 1, :] = top
            weights.append(jnp.exp2((s - top) * e).astype(BF16))
            keeps.append(jnp.exp2((old - top) * e))
        values = jnp.concatenate([values.T, jnp.ones((8, T), BF16)], axis=0)
        for n, (p, keep) in enumerate(zip(weights, keeps)):
            mix_s[n] = mix_s[n] * keep + _dot(values, p, 1, 0)

    def attend(i):
        blocks = 2 * z + 2
        h, j = i // blocks, i % blocks
        odd = j % 2
        src = 2 * (z - j // 2) + jnp.where(odd == 0, c, 1 - c)

        @pl.when(odd == 1)
        def _():
            kv_across(src, h, 0).wait_recv()

        @pl.when(j == 0)
        def _():
            top_s[...] = jnp.full((8, T), NEG, F32)
            mix_s[...] = jnp.zeros((8, HEAD + 8, T), F32)
            block(h, src, True)

        pl.when((j > 0) & (src < sp))(lambda: block(h, src, False))

        @pl.when(j == blocks - 1)
        def _():
            for n in range(8):
                at = pl.ds(pl.multiple_of(h * WIDE + n * HEAD, HEAD), HEAD)
                lhs_s[1, :, at] = (mix_s[n, :HEAD, :] * (1 / mix_s[n, HEAD : HEAD + 1, :])).T.astype(BF16)

    handlers = ((OWN, send_own), (Z_IN, z_in), (XY_OUT, unless_direct(xy_out)), (XY_IN, unless_direct(xy_in)), (D_IN, d_in_and_sent),
                (TAKE, load_unit), (KV_OUT, kv_out), (KV_IN, kv_in), (ATTEND, attend), (NORM, lambda i: norm()), (WORK, work_unit))

    def seven(g, counts):
        at, word = z * len(ORDERS[0]) + g, jnp.int32(0)
        for n, number in enumerate(sum(ORDERS, ())):
            word = jnp.where(at == n, number, word)

        def one(_, state):
            word, counts = state[0], state[1:]
            op = word % 16
            for (code, handler), count in zip(handlers, counts):
                pl.when(op == code)(functools.partial(handler, count))
            return (word // 16, *(count + jnp.where(op == code, 1, 0) for (code, _), count in zip(handlers, counts)))

        return lax.fori_loop(0, 7, one, (word, *counts))[1:]

    lax.fori_loop(0, len(ORDERS[0]), seven, (jnp.int32(0),) * len(handlers))

    lax.fori_loop(PHASES - BEHIND, PHASES, own_sent, None)
    lax.fori_loop(SLOTS - LATE, SLOTS, sent, None)

    def kv_sent(h, _):
        for j in range(4):
            @pl.when(z >= j)
            def _():
                pl.when(z < 3)(lambda: kv_up(sp - 2 * j, h, j).wait_send())
                kv_across(sp - 2 * j, h, j).wait_send()

    lax.fori_loop(0, 4, kv_sent, None)


def solution(mesh):
    dma = pltpu.SemaphoreType.DMA

    def step(x, gain, wq, wk, wv, wo):
        rate = THETA ** (-jnp.arange(HEAD // 2, dtype=F32) / (HEAD // 2))
        rate = jnp.concatenate([rate, rate])[None]
        hbm, vmem = pl.BlockSpec(memory_space=pltpu.HBM), pl.BlockSpec(memory_space=pltpu.VMEM)
        y, _ = pl.pallas_call(
            _kernel,
            in_specs=[hbm, vmem, hbm, hbm, hbm, hbm, vmem],
            out_specs=[vmem, hbm],
            out_shape=[pltpu.VMEM((T, D), BF16), jax.ShapeDtypeStruct((PHASES, 4, 2 * T, WIDE), BF16)],
            scratch_shapes=[
                pltpu.VMEM((T, D), BF16), pltpu.VMEM((2, T, D), BF16), pltpu.VMEM((32, T, HEAD), BF16), pltpu.VMEM((8, 4, 2, T, HEAD), BF16),
                pltpu.VMEM((T, D), F32), pltpu.VMEM((2, 2 * T, WIDE), BF16), pltpu.VMEM((8, HEAD + 8, T), F32), pltpu.VMEM((8, T), F32),
                pltpu.VMEM((T, HEAD), F32), pltpu.VMEM((T, HEAD), F32),
                *[dma((PHASES, 4))] * 6, *[dma((SLOTS,))] * 6, *[dma((PHASES,))] * 3,
                dma((2,)), dma((4, 4)), dma((4, 4)), dma((4, 4)), dma((4, 4)), dma((2,)), dma((1,)),
            ],
            compiler_params=pltpu.CompilerParams(collective_id=0, has_side_effects=True, vmem_limit_bytes=VMEM),
            cost_estimate=pl.CostEstimate(flops=2 * T * D * (2 * D + 1024) + 4 * T * D * D, transcendentals=32 * T * D, bytes_accessed=2**28),
        )(x, gain, wk, wv, wq, wo, rate)
        return y

    tokens, whole = P(("dp", "sp"), None), P("sp", None)
    return jax.shard_map(
        step,
        mesh=mesh,
        in_specs=(tokens, P(None), whole, whole, whole, whole),
        out_specs=tokens,
        check_vma=False,
    )
```
